32 devices in a mesh: partner: 8 (over y, x, core), block: 4 (over z).
Axes of the slice: x: 2, y: 2, z: 4, core: 2. Of those that a mesh axis runs over, the one named last changes fastest.
Arguments:
- points: bfloat16 [32, 32768], P(None, ('partner', 'block')), may hold values from -6 to 6
- tree_order: int32 [32768], P(('partner', 'block')), may hold values from 0 to 32767, as said below
- nearby_dense_blocks: bfloat16 [256, 3, 128, 128], P(('partner', 'block')), may hold values from -0.3125 to 0.3125
- neighbours: int32 [256, 3], P(('partner', 'block')), may hold values from 0 to 255, as said below
- compress: bfloat16 [256, 128, 128], P(('partner', 'block')), may hold values from -0.5 to 0.5
- expand: bfloat16 [256, 128, 128], P(('partner', 'block')), may hold values from -0.5 to 0.5
- top_factor: bfloat16 [256, 128, 128], P(('partner', 'block')), may hold values from -0.5 to 0.5
- butterfly_mixers: bfloat16 [2, 256, 2, 128, 128], P(None, ('partner', 'block')), may hold values from -0.375 to 0.375
- block_map: int32 [3, 8], replicated, may hold values from 0 to 7, as said below
Outputs:
- applied: bfloat16 [32, 32768], P(None, ('partner', 'block'))
The draws below stay inside these ranges and needn't reach their ends.
Inputs may be any that keep to these rules, and one draw needn't show every extreme that they name: tree_order[r] lies among the 1024 points of the aligned group of 1024 rows that holds r, and names every point once. neighbours[l, 0] is l; every other entry lies within 2 leaves of l and in the same aligned group of 32 leaves as l. `block_map`: each row names exactly 4 different slots, each of them twice.
All inputs are finite; a program needn't handle non-finite values.
Results may differ from the reference program's by a relative error of at most 0.001.
Values may be sent and summed in bfloat16 or wider, within the bound.
No kernel may reach another device: no remote copies, remote signals or barrier semaphores. Data moves between devices by JAX's collectives and lax.ppermute only.
A program may use at most 64 MiB of HBM per device.

```python
import jax
import jax.numpy as jnp
from jax import lax

NV = 32
LEAF = 128
KB = 128
NB = 3
REACH = 2
PTS_DEV = 1024
LEAVES_DEV = 8
LEVELS = 3
MIXS = 2
POINTS = 32768
LEAVES = 256
N_PARTNER = 8
N_BLOCK = 4


def draw_tree_order(key, part):
    key = jax.random.fold_in(key, 11)
    devices = N_PARTNER * N_BLOCK
    keys = jax.random.split(key, devices)
    rows = jax.vmap(lambda single: jax.random.permutation(single, PTS_DEV))(keys)
    offsets = (jnp.arange(devices, dtype=jnp.int32) * PTS_DEV)[:, None]
    return (rows.astype(jnp.int32) + offsets).reshape(-1).astype(jnp.int32)


def draw_neighbours(key, part):
    key = jax.random.fold_in(key, 23)
    leaf_numbers = jnp.arange(LEAVES, dtype=jnp.int32)[:, None]
    span = LEAVES_DEV * N_BLOCK
    lowest = leaf_numbers // span * span
    offsets = jax.random.randint(key, (LEAVES, NB - 1), -REACH, REACH + 1, dtype=jnp.int32)
    others = jnp.clip(leaf_numbers + offsets, lowest, lowest + span - 1)
    return jnp.concatenate([leaf_numbers, others], axis=1).astype(jnp.int32)


def draw_block_map(key, part):
    key = jax.random.fold_in(key, 37)

    def one_row(single):
        first, second = jax.random.split(single)
        middle = 1 + jax.random.permutation(first, LEAVES_DEV - 2)[:LEAVES_DEV // 2 - 2]
        ends = jnp.array([0, LEAVES_DEV - 1], dtype=jnp.int32)
        chosen = jnp.concatenate([ends, middle.astype(jnp.int32)])
        doubled = jnp.concatenate([chosen, chosen])
        return jnp.take(doubled, jax.random.permutation(second, LEAVES_DEV))
    return jax.vmap(one_row)(jax.random.split(key, LEVELS)).astype(jnp.int32)


def shard_levels(rng, extent, shards, least, top_value):
    def one(dim, parts):
        heights = jax.random.uniform(jax.random.fold_in(jax.random.fold_in(rng, 6), dim), (parts,), jnp.float32, least / len(shards), top_value / len(shards))
        return jnp.repeat(jnp.exp(heights), extent[dim] // parts).reshape((-1,) + (1,) * (len(extent) - dim - 1))

    factor_of = one(*shards[0])
    for cut in shards[1:]:
        factor_of = factor_of * one(*cut)
    return factor_of


def normal_values(own_key, shape, spread, reach, cuts=(), kind=jnp.bfloat16):
    values = spread * jax.random.normal(own_key, shape, jnp.float32)
    if cuts:
        values = values * shard_levels(own_key, shape, cuts, -0.22, 0.18)
    return jnp.clip(values, -reach, reach).astype(kind)


def setup_inputs(seed: int = 0) -> dict:
    key_list = jax.random.split(jax.random.key(seed), 10)
    points = normal_values(key_list[0], (NV, POINTS), 1.0, 6.0, ((1, 32),))
    tree_order = draw_tree_order(jax.random.fold_in(key_list[9], 71), 0)
    nearby_dense_blocks = normal_values(key_list[2], (LEAVES, NB, LEAF, LEAF), (NB * LEAF) ** -0.5, 0.3125, ((0, 32),))
    neighbours = draw_neighbours(jax.random.fold_in(key_list[9], 71), 0)
    compress = normal_values(key_list[4], (LEAVES, LEAF, KB), LEAF ** -0.5, 0.5, ((0, 32),))
    expand = normal_values(key_list[5], (LEAVES, KB, LEAF), KB ** -0.5, 0.5, ((0, 32),))
    top_factor = normal_values(key_list[6], (LEAVES, KB, KB), KB ** -0.5, 0.5, ((0, 32),))
    butterfly_mixers = normal_values(key_list[7], (MIXS, LEAVES, 2, KB, KB), (2 * KB) ** -0.5, 0.375, ((1, 32),))
    block_map = draw_block_map(jax.random.fold_in(key_list[9], 71), 0)
    return dict(points=points, tree_order=tree_order, nearby_dense_blocks=nearby_dense_blocks, neighbours=neighbours, compress=compress, expand=expand, top_factor=top_factor, butterfly_mixers=butterfly_mixers, block_map=block_map)


HI = lax.Precision.HIGHEST


def swap_partner(state, bit):
    count = state.shape[0]
    grouped = state.reshape((count >> (bit + 1), 2, 1 << bit) + state.shape[1:])
    return jnp.flip(grouped, axis=1).reshape(state.shape)


def per_partner(func, *arrays):
    return lax.map(lambda pieces: func(*pieces), arrays)


def reference(points, tree_order, nearby_dense_blocks, neighbours, compress, expand, top_factor, butterfly_mixers, block_map):
    n_part = N_PARTNER
    n_blk = N_BLOCK
    ordered = jnp.take(points, tree_order, axis=0 + 1)
    leaf_rows = ordered.reshape(NV, LEAVES, LEAF).transpose(1, 0, 2)
    gathered = jnp.take(leaf_rows, neighbours.reshape(-1), axis=0).reshape(n_part, n_blk * LEAVES_DEV, NB, NV, LEAF)
    near_view = nearby_dense_blocks.reshape(n_part, n_blk * LEAVES_DEV, NB, LEAF, LEAF)

    def nearby_single_block(source, blocks):
        return jnp.einsum("lnvs,lnst->lvt", source.astype(jnp.float32), blocks.astype(jnp.float32))

    nearby_field_sum = per_partner(nearby_single_block, gathered, near_view).reshape(n_part, n_blk, LEAVES_DEV, NV, LEAF)

    own_rows = leaf_rows.reshape(n_part, n_blk, LEAVES_DEV, NV, LEAF)
    comp_view = compress.reshape(n_part, n_blk, LEAVES_DEV, LEAF, KB)

    def compress_one(rows, factor):
        return jnp.einsum("qbvs,qbsk->qbvk", rows.astype(jnp.float32), factor.astype(jnp.float32))

    state = per_partner(compress_one, own_rows, comp_view)

    other = jnp.take(swap_partner(state, LEVELS - 1), block_map[0], axis=2)
    top_view = top_factor.reshape(n_part, n_blk, LEAVES_DEV, KB, KB)

    def top_one(coeffs, factor):
        return jnp.einsum("qbvk,qbkj->qbvj", coeffs, factor.astype(jnp.float32), precision=HI)

    state = per_partner(top_one, other, top_view)

    for section in range(LEVELS - 1):
        bit = LEVELS - 2 - section
        other = jnp.take(swap_partner(state, bit), block_map[section + 1], axis=2)
        mix_view = butterfly_mixers[section].reshape(n_part, n_blk, LEAVES_DEV, 2, KB, KB)

        def mix_one(own, across_partners, factor):
            widened = factor.astype(jnp.float32)
            first = jnp.einsum("qbvk,qbkj->qbvj", own, widened[:, :, 0], precision=HI)
            second = jnp.einsum("qbvk,qbkj->qbvj", across_partners, widened[:, :, 1], precision=HI)
            return first + second

        state = per_partner(mix_one, state, other, mix_view)

    exp_view = expand.reshape(n_part, n_blk, LEAVES_DEV, KB, LEAF)

    def expand_one(coeffs, factor):
        return jnp.einsum("qbvk,qbks->qbvs", coeffs, factor.astype(jnp.float32), precision=HI)

    far_field = per_partner(expand_one, state, exp_view)
    in_tree = (nearby_field_sum + far_field).astype(jnp.bfloat16)
    in_tree = in_tree.transpose(3, 0, 1, 2, 4).reshape(NV, POINTS)
    applied = jnp.zeros((NV, POINTS), jnp.bfloat16)
    return applied.at[:, tree_order].set(in_tree)
```

```python
import functools

import jax
import jax.numpy as jnp
from jax import lax
from jax.experimental import pallas as pl
from jax.experimental.pallas import tpu as pltpu
from jax.sharding import PartitionSpec as P

REACH = 2
LANES = 128
VMEM = pl.BlockSpec(memory_space=pltpu.VMEM)
SMEM = pl.BlockSpec(memory_space=pltpu.SMEM)
ANY = pl.BlockSpec(memory_space=pl.ANY)


def call(body, outs, in_specs, scratch=(), flops=1 << 20, moved=1 << 18, name=None):
    single = not isinstance(outs, (list, tuple))
    return pl.pallas_call(
        body,
        out_shape=outs,
        in_specs=in_specs,
        out_specs=VMEM if single else [VMEM] * len(outs),
        scratch_shapes=list(scratch),
        compiler_params=pltpu.CompilerParams(vmem_limit_bytes=16 << 20),
        cost_estimate=pl.CostEstimate(flops=flops, bytes_accessed=moved, transcendentals=0),
        name=name,
    )


def tables(map_ref, row, slot_ref, rank_ref, slots):
    mask = jnp.int32(0)
    for i in range(slots):
        mask = mask | (jnp.int32(1) << map_ref[row, i])
    rank = jnp.int32(0)
    for j in range(slots):
        slot_ref[rank] = jnp.int32(j)
        rank_ref[j] = rank
        rank = rank + ((mask >> j) & 1)


def split(x):
    high = x.astype(jnp.bfloat16)
    low = (x - high.astype(jnp.float32)).astype(jnp.bfloat16)
    return jnp.concatenate([high, low], axis=0)


def times(pair, factor):
    both = jnp.dot(pair, factor, preferred_element_type=jnp.float32)
    rows = both.shape[0] // 2
    return both[:rows] + both[rows:]


def pick_lanes(blocks, high, low):
    rows = blocks[0].shape[0]
    high = jnp.broadcast_to(high, (rows, LANES))
    low = jnp.broadcast_to(low, (rows, LANES))
    out = jnp.take_along_axis(blocks[0], low, axis=1)
    for b in range(1, len(blocks)):
        out = jnp.where(high == b, jnp.take_along_axis(blocks[b], low, axis=1), out)
    return out


def column_blocks(x, leaves):
    return [x[:, b * LANES : (b + 1) * LANES].astype(jnp.float32) for b in range(leaves)]


def first_body(points, order, compress, block_map, sent, pts, idx, comp, table, slot, rank, sems):
    leaves = idx.shape[0]
    copies = [
        pltpu.make_async_copy(block_map, table, sems.at[0]),
        pltpu.make_async_copy(order, idx, sems.at[1]),
        pltpu.make_async_copy(points, pts, sems.at[2]),
        pltpu.make_async_copy(compress, comp, sems.at[3]),
    ]
    for copy in copies:
        copy.start()
    copies[0].wait()
    tables(table, 0, slot, rank, leaves)
    copies[1].wait()
    copies[2].wait()
    blocks = column_blocks(pts[...], leaves)
    rows = []
    for k in range(leaves // 2):
        local = idx[pl.ds(slot[k], 1), :] & (leaves * LANES - 1)
        rows.append(pick_lanes(blocks, local >> 7, local & (LANES - 1)).astype(jnp.bfloat16))
    copies[3].wait()
    for k in range(leaves // 2):
        sent[k] = split(jnp.dot(rows[k], comp[slot[k]], preferred_element_type=jnp.float32))


def order_body(points, order, ordered, head, tail):
    leaves = order.shape[0]
    blocks = column_blocks(points[...], leaves)
    for leaf in range(leaves):
        local = order[pl.ds(leaf, 1), :] & (leaves * LANES - 1)
        rows = pick_lanes(blocks, local >> 7, local & (LANES - 1)).astype(jnp.bfloat16)
        ordered[leaf] = rows
        if leaf < REACH:
            head[leaf] = rows
        if leaf >= leaves - REACH:
            tail[leaf - leaves + REACH] = rows


def near_body(base, near, before, ordered, after, blocks, order, field, place, windows):
    leaves, near_count = blocks.shape[0], blocks.shape[1]
    windows[pl.ds(0, REACH)] = before[...]
    windows[pl.ds(REACH, leaves)] = ordered[...]
    windows[pl.ds(REACH + leaves, REACH)] = after[...]
    for leaf in range(leaves):
        total = None
        for n in range(near_count):
            source = windows[near[leaf, n] - base[0] + REACH]
            term = jnp.dot(source, blocks[leaf, n], preferred_element_type=jnp.float32)
            total = term if total is None else total + term
        field[leaf] = total
    count = leaves * LANES
    target = lax.broadcasted_iota(jnp.int32, (count, LANES), 0)
    kind = lax.broadcasted_iota(jnp.int32, (8, LANES), 0)
    lane = lax.broadcasted_iota(jnp.int32, (8, LANES), 1)
    total = None
    for leaf in range(leaves):
        local = order[pl.ds(leaf, 1), :] & (count - 1)
        hit = jnp.where(target == local, 1.0, 0.0).astype(jnp.bfloat16)
        value = jnp.where(kind == 0, leaf, lane).astype(jnp.float32).astype(jnp.bfloat16)
        term = lax.dot_general(
            value, hit, (((1,), (1,)), ((), ())), preferred_element_type=jnp.float32
        )
        total = term if total is None else total + term
    place[...] = total.astype(jnp.int32)


def top_send_body(block_map, received, factor, sent, slot, rank, slot_next, rank_next):
    leaves = factor.shape[0]
    tables(block_map, 0, slot, rank, leaves)
    tables(block_map, 1, slot_next, rank_next, leaves)
    for k in range(leaves // 2):
        i = slot_next[k]
        sent[k] = split(times(received[rank[block_map[0, i]]], factor[i]))


def top_own_body(block_map, received, factor, mixers, own, slot, rank):
    leaves = factor.shape[0]
    tables(block_map, 0, slot, rank, leaves)
    for i in range(leaves):
        state = split(times(received[rank[block_map[0, i]]], factor[i]))
        own[i] = times(state, mixers[0, i, 0])


def mix_send_body(level, block_map, received, own, mixers, sent, slot, rank, slot_next, rank_next):
    leaves = own.shape[0]
    tables(block_map, level, slot, rank, leaves)
    tables(block_map, level + 1, slot_next, rank_next, leaves)
    for k in range(leaves // 2):
        i = slot_next[k]
        other = times(received[rank[block_map[level, i]]], mixers[level - 1, i, 1])
        sent[k] = split(own[i] + other)


def mix_own_body(level, block_map, received, own, mixers, own_next, slot, rank):
    leaves = own.shape[0]
    tables(block_map, level, slot, rank, leaves)
    for i in range(leaves):
        other = times(received[rank[block_map[level, i]]], mixers[level - 1, i, 1])
        own_next[i] = times(split(own[i] + other), mixers[level, i, 0])


def last_body(level, block_map, received, own, mixers, expand, field, place, applied, slot, rank):
    leaves = own.shape[0]
    tables(block_map, level, slot, rank, leaves)
    blocks = []
    for i in range(leaves):
        other = times(received[rank[block_map[level, i]]], mixers[level - 1, i, 1])
        far = times(split(own[i] + other), expand[i])
        blocks.append((field[i] + far).astype(jnp.bfloat16).astype(jnp.float32))
    for b in range(leaves):
        high = place[pl.ds(0, 1), b * LANES : (b + 1) * LANES]
        low = place[pl.ds(1, 1), b * LANES : (b + 1) * LANES]
        applied[:, b * LANES : (b + 1) * LANES] = pick_lanes(blocks, high, low).astype(jnp.bfloat16)


def from_partner(x, axis, bit):
    return lax.ppermute(x, axis, [(i, i ^ 1 << bit) for i in range(lax.axis_size(axis))])


def on_device(
    points,
    tree_order,
    nearby_dense_blocks,
    neighbours,
    compress,
    expand,
    top_factor,
    butterfly_mixers,
    block_map,
):
    vectors, count = points.shape
    leaves = nearby_dense_blocks.shape[0]
    levels = lax.axis_size("partner").bit_length() - 1
    half = leaves // 2
    device = lax.axis_index("partner") * lax.axis_size("block") + lax.axis_index("block")
    base = (device * leaves).astype(jnp.int32).reshape(1)
    order = tree_order.reshape(leaves, LANES)
    ints = pltpu.SMEM((leaves + 1,), jnp.int32)
    pair = jax.ShapeDtypeStruct((half, 2 * vectors, LANES), jnp.bfloat16)
    state = jax.ShapeDtypeStruct((leaves, vectors, LANES), jnp.float32)
    edge = jax.ShapeDtypeStruct((REACH, vectors, LANES), jnp.bfloat16)

    sent = call(
        first_body,
        pair,
        [ANY, ANY, ANY, ANY],
        [
            pltpu.VMEM(points.shape, points.dtype),
            pltpu.VMEM(order.shape, order.dtype),
            pltpu.VMEM(compress.shape, compress.dtype),
            pltpu.SMEM(block_map.shape, block_map.dtype),
            ints,
            ints,
            pltpu.SemaphoreType.DMA((4,)),
        ],
        name="first",
    )(points, order, compress, block_map)
    received = from_partner(sent, "partner", levels - 1)

    ordered, head, tail = call(
        order_body,
        [jax.ShapeDtypeStruct((leaves, vectors, LANES), jnp.bfloat16), edge, edge],
        [VMEM, VMEM],
        flops=1 << 24,
        name="order",
    )(points, order)
    ends = lax.axis_size("block") - 1
    before = lax.ppermute(tail, "block", [(i, i + 1) for i in range(ends)])
    after = lax.ppermute(head, "block", [(i + 1, i) for i in range(ends)])

    sent = call(
        top_send_body, pair, [SMEM, VMEM, VMEM], [ints] * 4, name="top_send"
    )(block_map, received, top_factor)
    own = call(
        top_own_body, state, [SMEM, VMEM, VMEM, VMEM], [ints] * 2, flops=1 << 24, name="top_own"
    )(block_map, received, top_factor, butterfly_mixers)
    field, place = call(
        near_body,
        [state, jax.ShapeDtypeStruct((8, count), jnp.int32)],
        [SMEM, SMEM, VMEM, VMEM, VMEM, VMEM, VMEM],
        [pltpu.VMEM((leaves + 2 * REACH, vectors, LANES), jnp.bfloat16)],
        flops=1 << 25,
        name="near",
    )(base, neighbours, before, ordered, after, nearby_dense_blocks, order)

    for level in range(1, levels):
        received = from_partner(sent, "partner", levels - 1 - level)
        if level < levels - 1:
            sent = call(
                functools.partial(mix_send_body, level),
                pair,
                [SMEM, VMEM, VMEM, VMEM],
                [ints] * 4,
                name="mix_send",
            )(block_map, received, own, butterfly_mixers)
            own = call(
                functools.partial(mix_own_body, level),
                state,
                [SMEM, VMEM, VMEM, VMEM],
                [ints] * 2,
                flops=1 << 24,
                name="mix_own",
            )(block_map, received, own, butterfly_mixers)
    return call(
        functools.partial(last_body, levels - 1),
        jax.ShapeDtypeStruct(points.shape, points.dtype),
        [SMEM] + [VMEM] * 6,
        [ints] * 2,
        name="last",
    )(block_map, received, own, butterfly_mixers, expand, field, place)


def solution(mesh):
    return jax.shard_map(
        on_device,
        mesh=mesh,
        in_specs=(
            P(None, ("partner", "block")),
            P(("partner", "block")),
            P(("partner", "block"), None, None, None),
            P(("partner", "block"), None),
            P(("partner", "block"), None, None),
            P(("partner", "block"), None, None),
            P(("partner", "block"), None, None),
            P(None, ("partner", "block"), None, None, None),
            P(),
        ),
        out_specs=P(None, ("partner", "block")),
        check_vma=False,
    )
```

```python
import functools

import jax
import jax.numpy as jnp
from jax import lax
from jax.experimental import pallas as pl
from jax.experimental.pallas import tpu as pltpu
from jax.sharding import PartitionSpec as P


REACH = 2
LANES = 128
VMEM = pl.BlockSpec(memory_space=pltpu.VMEM)
HBM = pl.BlockSpec(memory_space=pltpu.HBM)


def call(body, outs, in_specs, scratch=(), flops=1 << 20, moved=1 << 18):
    single = not isinstance(outs, (list, tuple))
    run = pl.pallas_call(
        body,
        out_shape=outs,
        in_specs=in_specs,
        out_specs=VMEM if single else [VMEM] * len(outs),
        scratch_shapes=list(scratch),
        compiler_params=pltpu.CompilerParams(vmem_limit_bytes=16 << 20),
        cost_estimate=pl.CostEstimate(flops=flops, bytes_accessed=moved, transcendentals=0),
    )

    def bound(*args):
        return run(
            *[
                pltpu.with_memory_space_constraint(a, pltpu.HBM) if s is HBM else a
                for a, s in zip(args, in_specs)
            ]
        )

    return bound


def tables(map_ref, row, slot_ref, rank_ref, slots):
    mask = jnp.int32(0)
    for i in range(slots):
        mask = mask | (jnp.int32(1) << map_ref[row, i])
    rank = jnp.int32(0)
    for j in range(slots):
        slot_ref[rank] = jnp.int32(j)
        rank_ref[j] = rank
        rank = rank + ((mask >> j) & 1)


class Places:
    def __init__(self, levels, leaves, near_count):
        self.leaves, self.half = leaves, leaves // 2
        self.level_rows = leaves + 2 * self.half
        self.near_base = levels * self.level_rows
        self.near_count = near_count
        self.rows = -(-(self.near_base + leaves * near_count) // 8) * 8

    def piece(self, level, i):
        return level * self.level_rows + i

    def slot(self, level, k):
        return level * self.level_rows + self.leaves + k

    def slot_piece(self, level, k):
        return level * self.level_rows + self.leaves + self.half + k

    def near(self, leaf, n):
        return self.near_base + leaf * self.near_count + n


def read(table, row):
    return table[pl.ds(row, 1), :][0, 0]


def split(x):
    high = x.astype(jnp.bfloat16)
    low = (x - high.astype(jnp.float32)).astype(jnp.bfloat16)
    return jnp.concatenate([high, low], axis=0)


def times(pair, factor):
    both = jnp.dot(pair, factor, preferred_element_type=jnp.float32)
    rows = both.shape[0] // 2
    return both[:rows] + both[rows:]


def pick_lanes(blocks, high, low):
    rows = blocks[0].shape[0]
    high = jnp.broadcast_to(high, (rows, LANES))
    low = jnp.broadcast_to(low, (rows, LANES))
    out = jnp.take_along_axis(blocks[0], low, axis=1)
    for b in range(1, len(blocks)):
        out = jnp.where(high == b, jnp.take_along_axis(blocks[b], low, axis=1), out)
    return out


def column_blocks(x, leaves):
    return [x[:, b * LANES : (b + 1) * LANES].astype(jnp.float32) for b in range(leaves)]


def first_body(points, order, compress, block_map, sent, pts, idx, comp, table, slot, rank, sems):
    leaves = idx.shape[0]
    copies = [
        pltpu.make_async_copy(block_map, table, sems.at[0]),
        pltpu.make_async_copy(order, idx, sems.at[1]),
        pltpu.make_async_copy(points, pts, sems.at[2]),
        pltpu.make_async_copy(compress, comp, sems.at[3]),
    ]
    for copy in copies:
        copy.start()
    copies[0].wait()
    tables(table, 0, slot, rank, leaves)
    copies[1].wait()
    copies[2].wait()
    blocks = column_blocks(pts[...], leaves)
    rows = []
    for k in range(leaves // 2):
        local = idx[pl.ds(slot[k], 1), :] & (leaves * LANES - 1)
        rows.append(pick_lanes(blocks, local >> 7, local & (LANES - 1)).astype(jnp.bfloat16))
    copies[3].wait()
    for k in range(leaves // 2):
        sent[k] = split(jnp.dot(rows[k], comp[slot[k]], preferred_element_type=jnp.float32))


def order_body(
    places, points, order, block_map, near, ordered, even, odd, table, maps, nears, slot, rank, sems
):
    leaves = order.shape[0]
    levels = maps.shape[0]
    copies = [
        pltpu.make_async_copy(block_map, maps, sems.at[0]),
        pltpu.make_async_copy(near, nears, sems.at[1]),
    ]
    for copy in copies:
        copy.start()
    blocks = column_blocks(points[...], leaves)
    for leaf in range(leaves):
        local = order[pl.ds(leaf, 1), :] & (leaves * LANES - 1)
        ordered[leaf] = pick_lanes(blocks, local >> 7, local & (LANES - 1)).astype(jnp.bfloat16)
    block = lax.axis_index("block")
    parity = block & 1
    head, tail = 0, leaves - REACH
    even[...] = ordered[pl.ds(jnp.where(parity == 0, tail, head), REACH)]
    odd[...] = ordered[pl.ds(jnp.where(parity == 0, head, tail), REACH)]
    base = (lax.axis_index("partner") * lax.axis_size("block") + block) * leaves

    def put(row, value):
        table[pl.ds(row, 1), :] = jnp.full((1, LANES), value, jnp.int32)

    for copy in copies:
        copy.wait()
    for level in range(levels):
        tables(maps, level, slot, rank, leaves)
        for i in range(leaves):
            put(places.piece(level, i), rank[maps[level, i]])
        if level > 0:
            for k in range(leaves // 2):
                i = slot[k]
                put(places.slot(level, k), i)
                put(places.slot_piece(level, k), read(table, places.piece(level - 1, i)))
    for leaf in range(leaves):
        for n in range(nears.shape[0]):
            put(places.near(leaf, n), nears[n, leaf] - base + REACH)


def near_body(places, table, even, ordered, odd, blocks, order, field, place, windows):
    leaves, near_count = blocks.shape[0], blocks.shape[1]
    parity = lax.axis_index("block") & 1
    first, last = 0, leaves + REACH
    windows[pl.ds(jnp.where(parity == 0, last, first), REACH)] = even[...]
    windows[pl.ds(jnp.where(parity == 0, first, last), REACH)] = odd[...]
    windows[pl.ds(REACH, leaves)] = ordered[...]
    for leaf in range(leaves):
        total = None
        for n in range(near_count):
            source = windows[read(table, places.near(leaf, n))]
            term = jnp.dot(source, blocks[leaf, n], preferred_element_type=jnp.float32)
            total = term if total is None else total + term
        field[leaf] = total
    count = leaves * LANES
    target = lax.broadcasted_iota(jnp.int32, (count, LANES), 0)
    kind = lax.broadcasted_iota(jnp.int32, (8, LANES), 0)
    lane = lax.broadcasted_iota(jnp.int32, (8, LANES), 1)
    total = None
    for leaf in range(leaves):
        local = order[pl.ds(leaf, 1), :] & (count - 1)
        hit = jnp.where(target == local, 1.0, 0.0).astype(jnp.bfloat16)
        value = jnp.where(kind == 0, leaf, lane).astype(jnp.float32).astype(jnp.bfloat16)
        term = lax.dot_general(
            value, hit, (((1,), (1,)), ((), ())), preferred_element_type=jnp.float32
        )
        total = term if total is None else total + term
    place[...] = total.astype(jnp.int32)


def top_send_body(places, table, received, factor, sent):
    for k in range(sent.shape[0]):
        i = read(table, places.slot(1, k))
        sent[k] = split(times(received[read(table, places.slot_piece(1, k))], factor[i]))


def top_own_body(places, table, received, factor, mixers, own):
    for i in range(own.shape[0]):
        state = split(times(received[read(table, places.piece(0, i))], factor[i]))
        own[i] = times(state, mixers[0, i, 0])


def mix_send_body(places, level, table, received, own, mixers, sent):
    for k in range(sent.shape[0]):
        i = read(table, places.slot(level + 1, k))
        piece = received[read(table, places.slot_piece(level + 1, k))]
        sent[k] = split(own[i] + times(piece, mixers[level - 1, i, 1]))


def mix_own_body(places, level, table, received, own, mixers, own_next):
    for i in range(own.shape[0]):
        other = times(received[read(table, places.piece(level, i))], mixers[level - 1, i, 1])
        own_next[i] = times(split(own[i] + other), mixers[level, i, 0])


def last_body(places, level, table, received, own, mixers, expand, field, place, applied):
    leaves = own.shape[0]
    blocks = []
    for i in range(leaves):
        other = times(received[read(table, places.piece(level, i))], mixers[level - 1, i, 1])
        far = times(split(own[i] + other), expand[i])
        blocks.append((field[i] + far).astype(jnp.bfloat16).astype(jnp.float32))
    for b in range(leaves):
        high = place[pl.ds(0, 1), b * LANES : (b + 1) * LANES]
        low = place[pl.ds(1, 1), b * LANES : (b + 1) * LANES]
        applied[:, b * LANES : (b + 1) * LANES] = pick_lanes(blocks, high, low).astype(jnp.bfloat16)


def from_partner(x, bit):
    count = lax.axis_size("partner")
    return lax.ppermute(x, "partner", [(i, i ^ 1 << bit) for i in range(count)])


def with_neighbour(x, first):
    count = lax.axis_size("block")
    pairs = [(i, i + 1) for i in range(first, count - 1, 2)]
    return lax.ppermute(x, "block", pairs + [(b, a) for a, b in pairs])


def on_device(
    points,
    tree_order,
    nearby_dense_blocks,
    neighbours,
    compress,
    expand,
    top_factor,
    butterfly_mixers,
    block_map,
):
    vectors, count = points.shape
    leaves, near_count = neighbours.shape
    levels = lax.axis_size("partner").bit_length() - 1
    half = leaves // 2
    places = Places(levels, leaves, near_count)
    order = tree_order.reshape(leaves, LANES)
    ints = pltpu.SMEM((leaves + 1,), jnp.int32)
    pair = jax.ShapeDtypeStruct((half, 2 * vectors, LANES), jnp.bfloat16)
    state = jax.ShapeDtypeStruct((leaves, vectors, LANES), jnp.float32)
    edge = jax.ShapeDtypeStruct((REACH, vectors, LANES), jnp.bfloat16)
    part = functools.partial

    sent = call(
        first_body,
        pair,
        [HBM, HBM, HBM, HBM],
        [
            pltpu.VMEM(points.shape, points.dtype),
            pltpu.VMEM(order.shape, order.dtype),
            pltpu.VMEM(compress.shape, compress.dtype),
            pltpu.SMEM(block_map.shape, block_map.dtype),
            ints,
            ints,
            pltpu.SemaphoreType.DMA((4,)),
        ],
    )(points, order, compress, block_map)
    received = from_partner(sent, levels - 1)

    ordered, even, odd, table = call(
        part(order_body, places),
        [
            jax.ShapeDtypeStruct((leaves, vectors, LANES), jnp.bfloat16),
            edge,
            edge,
            jax.ShapeDtypeStruct((places.rows, LANES), jnp.int32),
        ],
        [VMEM, VMEM, HBM, HBM],
        [
            pltpu.SMEM(block_map.shape, block_map.dtype),
            pltpu.SMEM((near_count, leaves), neighbours.dtype),
            ints,
            ints,
            pltpu.SemaphoreType.DMA((2,)),
        ],
        flops=1 << 24,
    )(points, order, block_map, neighbours.T)
    even = with_neighbour(even, 0)
    odd = with_neighbour(odd, 1)

    sent = call(part(top_send_body, places), pair, [VMEM] * 3)(table, received, top_factor)
    own = call(part(top_own_body, places), state, [VMEM] * 4, flops=1 << 24)(
        table, received, top_factor, butterfly_mixers
    )
    field, place = call(
        part(near_body, places),
        [state, jax.ShapeDtypeStruct((8, count), jnp.int32)],
        [VMEM] * 6,
        [pltpu.VMEM((leaves + 2 * REACH, vectors, LANES), jnp.bfloat16)],
        flops=1 << 25,
    )(table, even, ordered, odd, nearby_dense_blocks, order)

    for level in range(1, levels):
        received = from_partner(sent, levels - 1 - level)
        if level < levels - 1:
            sent = call(part(mix_send_body, places, level), pair, [VMEM] * 4)(
                table, received, own, butterfly_mixers
            )
            own = call(
                part(mix_own_body, places, level), state, [VMEM] * 4, flops=1 << 24
            )(table, received, own, butterfly_mixers)
    return call(
        part(last_body, places, levels - 1),
        jax.ShapeDtypeStruct(points.shape, points.dtype),
        [VMEM] * 7,
    )(table, received, own, butterfly_mixers, expand, field, place)


def solution(mesh):
    return jax.shard_map(
        on_device,
        mesh=mesh,
        in_specs=(
            P(None, ("partner", "block")),
            P(("partner", "block")),
            P(("partner", "block"), None, None, None),
            P(("partner", "block"), None),
            P(("partner", "block"), None, None),
            P(("partner", "block"), None, None),
            P(("partner", "block"), None, None),
            P(None, ("partner", "block"), None, None, None),
            P(),
        ),
        out_specs=P(None, ("partner", "block")),
        check_vma=False,
    )
```

```python
import functools

import jax
import jax.numpy as jnp
from jax import lax
from jax.experimental import pallas as pl
from jax.experimental.pallas import tpu as pltpu
from jax.sharding import PartitionSpec as P


REACH = 2
LANES = 128
VMEM = pl.BlockSpec(memory_space=pltpu.VMEM)
HBM = pl.BlockSpec(memory_space=pltpu.HBM)


def call(body, outs, in_specs, scratch=(), flops=1 << 20, moved=1 << 18, place=VMEM):
    single = not isinstance(outs, (list, tuple))
    run = pl.pallas_call(
        body,
        out_shape=outs,
        in_specs=in_specs,
        out_specs=place if single else [VMEM] * len(outs),
        scratch_shapes=list(scratch),
        compiler_params=pltpu.CompilerParams(vmem_limit_bytes=16 << 20),
        cost_estimate=pl.CostEstimate(flops=flops, bytes_accessed=moved, transcendentals=0),
    )

    def bound(*args):
        return run(
            *[
                pltpu.with_memory_space_constraint(a, pltpu.HBM) if s is HBM else a
                for a, s in zip(args, in_specs)
            ]
        )

    return bound


def tables(map_ref, row, slot_ref, rank_ref, slots):
    mask = jnp.int32(0)
    for i in range(slots):
        mask = mask | (jnp.int32(1) << map_ref[row, i])
    rank = jnp.int32(0)
    for j in range(slots):
        slot_ref[rank] = jnp.int32(j)
        rank_ref[j] = rank
        rank = rank + ((mask >> j) & 1)


class Places:
    def __init__(self, levels, leaves, near_count):
        self.leaves, self.half = leaves, leaves // 2
        self.level_rows = leaves + 2 * self.half
        self.near_base = levels * self.level_rows
        self.near_count = near_count
        self.rows = -(-(self.near_base + leaves * near_count) // 8) * 8

    def piece(self, level, i):
        return level * self.level_rows + i

    def slot(self, level, k):
        return level * self.level_rows + self.leaves + k

    def slot_piece(self, level, k):
        return level * self.level_rows + self.leaves + self.half + k

    def near(self, leaf, n):
        return self.near_base + leaf * self.near_count + n


def read(table, row):
    return table[pl.ds(row, 1), :][0, 0]


def split(x):
    high = x.astype(jnp.bfloat16)
    low = (x - high.astype(jnp.float32)).astype(jnp.bfloat16)
    return jnp.concatenate([high, low], axis=0)


def times(pair, factor):
    both = jnp.dot(pair, factor, preferred_element_type=jnp.float32)
    rows = both.shape[0] // 2
    return both[:rows] + both[rows:]


def pick_lanes(blocks, high, low):
    rows = blocks[0].shape[0]
    high = jnp.broadcast_to(high, (rows, LANES))
    low = jnp.broadcast_to(low, (rows, LANES))
    out = jnp.take_along_axis(blocks[0], low, axis=1)
    for b in range(1, len(blocks)):
        out = jnp.where(high == b, jnp.take_along_axis(blocks[b], low, axis=1), out)
    return out


def column_blocks(x, leaves):
    return [x[:, b * LANES : (b + 1) * LANES].astype(jnp.float32) for b in range(leaves)]


def first_body(points, order, compress, block_map, sent, pts, idx, comp, table, slot, rank, sems):
    leaves = idx.shape[0]
    copies = [
        pltpu.make_async_copy(block_map, table, sems.at[0]),
        pltpu.make_async_copy(order, idx, sems.at[1]),
        pltpu.make_async_copy(points, pts, sems.at[2]),
        pltpu.make_async_copy(compress, comp, sems.at[3]),
    ]
    for copy in copies:
        copy.start()
    copies[0].wait()
    tables(table, 0, slot, rank, leaves)
    copies[1].wait()
    copies[2].wait()
    blocks = column_blocks(pts[...], leaves)
    rows = []
    for k in range(leaves // 2):
        local = idx[pl.ds(slot[k], 1), :] & (leaves * LANES - 1)
        rows.append(pick_lanes(blocks, local >> 7, local & (LANES - 1)).astype(jnp.bfloat16))
    copies[3].wait()
    for k in range(leaves // 2):
        sent[k] = split(jnp.dot(rows[k], comp[slot[k]], preferred_element_type=jnp.float32))


def order_body(
    places, points, order, block_map, near, mixers, dense,
    ordered, even, odd, table, mixers_out, dense_out, maps, nears, slot, rank, sems,
):
    leaves = order.shape[0]
    levels = maps.shape[0]
    copies = [
        pltpu.make_async_copy(block_map, maps, sems.at[0]),
        pltpu.make_async_copy(near, nears, sems.at[1]),
        pltpu.make_async_copy(mixers, mixers_out, sems.at[2]),
        pltpu.make_async_copy(dense, dense_out, sems.at[3]),
    ]
    for copy in copies:
        copy.start()
    blocks = column_blocks(points[...], leaves)
    for leaf in range(leaves):
        local = order[pl.ds(leaf, 1), :] & (leaves * LANES - 1)
        ordered[leaf] = pick_lanes(blocks, local >> 7, local & (LANES - 1)).astype(jnp.bfloat16)
    block = lax.axis_index("block")
    parity = block & 1
    head, tail = 0, leaves - REACH
    even[...] = ordered[pl.ds(jnp.where(parity == 0, tail, head), REACH)]
    odd[...] = ordered[pl.ds(jnp.where(parity == 0, head, tail), REACH)]
    base = (lax.axis_index("partner") * lax.axis_size("block") + block) * leaves

    def put(row, value):
        table[pl.ds(row, 1), :] = jnp.full((1, LANES), value, jnp.int32)

    copies[0].wait()
    copies[1].wait()
    for level in range(levels):
        tables(maps, level, slot, rank, leaves)
        for i in range(leaves):
            put(places.piece(level, i), rank[maps[level, i]])
        if level > 0:
            for k in range(leaves // 2):
                i = slot[k]
                put(places.slot(level, k), i)
                put(places.slot_piece(level, k), read(table, places.piece(level - 1, i)))
    for leaf in range(leaves):
        for n in range(nears.shape[0]):
            put(places.near(leaf, n), nears[n, leaf] - base + REACH)
    copies[2].wait()
    copies[3].wait()


def near_body(
    places, table, even, ordered, odd, blocks, order, mixers, expand, field, place, joint, windows
):
    leaves, near_count = blocks.shape[0], blocks.shape[1]
    parity = lax.axis_index("block") & 1
    first, last = 0, leaves + REACH
    windows[pl.ds(jnp.where(parity == 0, last, first), REACH)] = even[...]
    windows[pl.ds(jnp.where(parity == 0, first, last), REACH)] = odd[...]
    windows[pl.ds(REACH, leaves)] = ordered[...]
    for leaf in range(leaves):
        total = None
        for n in range(near_count):
            source = windows[read(table, places.near(leaf, n))]
            term = jnp.dot(source, blocks[leaf, n], preferred_element_type=jnp.float32)
            total = term if total is None else total + term
        field[leaf] = total
    count = leaves * LANES
    target = lax.broadcasted_iota(jnp.int32, (count, LANES), 0)
    kind = lax.broadcasted_iota(jnp.int32, (8, LANES), 0)
    lane = lax.broadcasted_iota(jnp.int32, (8, LANES), 1)
    total = None
    for leaf in range(leaves):
        local = order[pl.ds(leaf, 1), :] & (count - 1)
        hit = jnp.where(target == local, 1.0, 0.0).astype(jnp.bfloat16)
        value = jnp.where(kind == 0, leaf, lane).astype(jnp.float32).astype(jnp.bfloat16)
        term = lax.dot_general(
            value, hit, (((1,), (1,)), ((), ())), preferred_element_type=jnp.float32
        )
        total = term if total is None else total + term
    place[...] = total.astype(jnp.int32)
    for i in range(leaves):
        both = jnp.dot(mixers[mixers.shape[0] - 1, i, 1], expand[i], preferred_element_type=jnp.float32)
        high = both.astype(jnp.bfloat16)
        joint[i, :, :LANES] = high
        joint[i, :, LANES:] = (both - high.astype(jnp.float32)).astype(jnp.bfloat16)


def top_send_body(places, table, received, factor, sent):
    for k in range(sent.shape[0]):
        i = read(table, places.slot(1, k))
        sent[k] = split(times(received[read(table, places.slot_piece(1, k))], factor[i]))


def top_own_body(places, table, received, factor, mixers, own):
    for i in range(own.shape[0]):
        state = split(times(received[read(table, places.piece(0, i))], factor[i]))
        own[i] = times(state, mixers[0, i, 0])


def mix_send_body(places, level, table, received, own, mixers, sent):
    for k in range(sent.shape[0]):
        i = read(table, places.slot(level + 1, k))
        piece = received[read(table, places.slot_piece(level + 1, k))]
        sent[k] = split(own[i] + times(piece, mixers[level - 1, i, 1]))


def mix_own_body(places, level, table, received, own, mixers, own_next):
    for i in range(own.shape[0]):
        other = times(received[read(table, places.piece(level, i))], mixers[level - 1, i, 1])
        own_next[i] = times(split(own[i] + other), mixers[level, i, 0])


def base_body(places, level, table, received, own, mixers, expand, field, base):
    for i in range(own.shape[0]):
        if level:
            other = times(received[read(table, places.piece(level, i))], mixers[level - 1, i, 1])
            state = times(split(own[i] + other), mixers[level, i, 0])
        else:
            state = own[i]
        base[i] = field[i] + times(split(state), expand[i])


def last_body(places, level, table, received, base, joint, place, applied, rows, sems):
    leaves = base.shape[0]
    blocks = []
    for i in range(leaves):
        piece = received[read(table, places.piece(level, i))]
        far = jnp.dot(piece, joint[i], preferred_element_type=jnp.float32)
        half = far.shape[0] // 2
        far = (far[:half, :LANES] + far[half:, :LANES]) + (far[:half, LANES:] + far[half:, LANES:])
        blocks.append((base[i] + far).astype(jnp.bfloat16).astype(jnp.float32))
    group = rows.shape[0] // sems.shape[0]
    copies = []
    for g in range(sems.shape[0]):
        here = slice(g * group, (g + 1) * group)
        part = [block[here] for block in blocks]
        for b in range(leaves):
            lanes = slice(b * LANES, (b + 1) * LANES)
            picked = pick_lanes(part, place[pl.ds(0, 1), lanes], place[pl.ds(1, 1), lanes])
            rows[here, lanes] = picked.astype(jnp.bfloat16)
        copies.append(pltpu.make_async_copy(rows.at[here], applied.at[here], sems.at[g]))
        copies[-1].start()
    for copy in copies:
        copy.wait()


def from_partner(x, bit):
    count = lax.axis_size("partner")
    return lax.ppermute(x, "partner", [(i, i ^ 1 << bit) for i in range(count)])


def with_neighbour(x, first):
    count = lax.axis_size("block")
    to = list(range(count))
    for i in range(first, count - 1, 2):
        to[i], to[i + 1] = i + 1, i
    return lax.ppermute(x, "block", list(enumerate(to)))


def on_device(
    points,
    tree_order,
    nearby_dense_blocks,
    neighbours,
    compress,
    expand,
    top_factor,
    butterfly_mixers,
    block_map,
):
    vectors, count = points.shape
    leaves, near_count = neighbours.shape
    levels = lax.axis_size("partner").bit_length() - 1
    half = leaves // 2
    places = Places(levels, leaves, near_count)
    order = tree_order.reshape(leaves, LANES)
    ints = pltpu.SMEM((leaves + 1,), jnp.int32)
    pair = jax.ShapeDtypeStruct((half, 2 * vectors, LANES), jnp.bfloat16)
    state = jax.ShapeDtypeStruct((leaves, vectors, LANES), jnp.float32)
    edge = jax.ShapeDtypeStruct((REACH, vectors, LANES), jnp.bfloat16)
    part = functools.partial

    sent = call(
        first_body,
        pair,
        [HBM, HBM, HBM, HBM],
        [
            pltpu.VMEM(points.shape, points.dtype),
            pltpu.VMEM(order.shape, order.dtype),
            pltpu.VMEM(compress.shape, compress.dtype),
            pltpu.SMEM(block_map.shape, block_map.dtype),
            ints,
            ints,
            pltpu.SemaphoreType.DMA((4,)),
        ],
    )(points, order, compress, block_map)
    received = from_partner(sent, levels - 1)

    ordered, even, odd, table, mixers, dense = call(
        part(order_body, places),
        [
            jax.ShapeDtypeStruct((leaves, vectors, LANES), jnp.bfloat16),
            edge,
            edge,
            jax.ShapeDtypeStruct((places.rows, LANES), jnp.int32),
            jax.ShapeDtypeStruct(butterfly_mixers.shape, butterfly_mixers.dtype),
            jax.ShapeDtypeStruct(nearby_dense_blocks.shape, nearby_dense_blocks.dtype),
        ],
        [VMEM, VMEM, HBM, HBM, HBM, HBM],
        [
            pltpu.SMEM(block_map.shape, block_map.dtype),
            pltpu.SMEM((near_count, leaves), neighbours.dtype),
            ints,
            ints,
            pltpu.SemaphoreType.DMA((4,)),
        ],
        flops=1 << 24,
    )(points, order, block_map, neighbours.T, butterfly_mixers, nearby_dense_blocks)
    even = with_neighbour(even, 0)
    odd = with_neighbour(odd, 1)

    sent = call(part(top_send_body, places), pair, [VMEM] * 3)(table, received, top_factor)
    own = call(part(top_own_body, places), state, [VMEM] * 4, flops=1 << 24)(
        table, received, top_factor, mixers
    )
    field, place, joint = call(
        part(near_body, places),
        [
            state,
            jax.ShapeDtypeStruct((8, count), jnp.int32),
            jax.ShapeDtypeStruct((leaves, LANES, 2 * LANES), jnp.bfloat16),
        ],
        [VMEM] * 8,
        [pltpu.VMEM((leaves + 2 * REACH, vectors, LANES), jnp.bfloat16)],
        flops=1 << 25,
    )(table, even, ordered, odd, dense, order, mixers, expand)

    for level in range(1, levels):
        received = from_partner(sent, levels - 1 - level)
        if level < levels - 1:
            sent = call(part(mix_send_body, places, level), pair, [VMEM] * 4)(
                table, received, own, mixers
            )
            if level < levels - 2:
                own = call(
                    part(mix_own_body, places, level), state, [VMEM] * 4, flops=1 << 24
                )(table, received, own, mixers)
        if level == max(levels - 2, 1):
            base = call(
                part(base_body, places, level if levels > 2 else 0),
                state,
                [VMEM] * 6,
                flops=1 << 24,
            )(table, received, own, mixers, expand, field)
    return call(
        part(last_body, places, levels - 1),
        jax.ShapeDtypeStruct(points.shape, points.dtype),
        [VMEM] * 5,
        [pltpu.VMEM(points.shape, points.dtype), pltpu.SemaphoreType.DMA((4,))],
        place=HBM,
    )(table, received, base, joint, place)


def solution(mesh):
    return jax.shard_map(
        on_device,
        mesh=mesh,
        in_specs=(
            P(None, ("partner", "block")),
            P(("partner", "block")),
            P(("partner", "block"), None, None, None),
            P(("partner", "block"), None),
            P(("partner", "block"), None, None),
            P(("partner", "block"), None, None),
            P(("partner", "block"), None, None),
            P(None, ("partner", "block"), None, None, None),
            P(),
        ),
        out_specs=P(None, ("partner", "block")),
        check_vma=False,
    )
```

```python
import functools

import jax
import jax.numpy as jnp
from jax import lax
from jax.experimental import pallas as pl
from jax.experimental.pallas import tpu as pltpu
from jax.sharding import PartitionSpec as P


REACH = 2
LANES = 128
VMEM = pl.BlockSpec(memory_space=pltpu.VMEM)
HBM = pl.BlockSpec(memory_space=pltpu.HBM)


def call(body, outs, in_specs, scratch=(), flops=1 << 20, moved=1 << 18, place=VMEM):
    single = not isinstance(outs, (list, tuple))
    run = pl.pallas_call(
        body,
        out_shape=outs,
        in_specs=in_specs,
        out_specs=place if single else [VMEM] * len(outs),
        scratch_shapes=list(scratch),
        compiler_params=pltpu.CompilerParams(vmem_limit_bytes=16 << 20),
        cost_estimate=pl.CostEstimate(flops=flops, bytes_accessed=moved, transcendentals=0),
    )

    def bound(*args):
        return run(
            *[
                pltpu.with_memory_space_constraint(a, pltpu.HBM) if s is HBM else a
                for a, s in zip(args, in_specs)
            ]
        )

    return bound


def tables(map_ref, row, slot_ref, rank_ref, slots):
    mask = jnp.int32(0)
    for i in range(slots):
        mask = mask | (jnp.int32(1) << map_ref[row, i])
    rank = jnp.int32(0)
    for j in range(slots):
        slot_ref[rank] = jnp.int32(j)
        rank_ref[j] = rank
        rank = rank + ((mask >> j) & 1)


class Places:
    def __init__(self, levels, leaves, near_count):
        self.leaves, self.half = leaves, leaves // 2
        self.level_rows = leaves + 2 * self.half
        self.near_base = levels * self.level_rows
        self.near_count = near_count
        self.rows = -(-(self.near_base + leaves * near_count) // 8) * 8

    def piece(self, level, i):
        return level * self.level_rows + i

    def slot(self, level, k):
        return level * self.level_rows + self.leaves + k

    def slot_piece(self, level, k):
        return level * self.level_rows + self.leaves + self.half + k

    def near(self, leaf, n):
        return self.near_base + leaf * self.near_count + n


def read(table, row):
    return table[pl.ds(row, 1), :][0, 0]


def split(x):
    high = x.astype(jnp.bfloat16)
    low = (x - high.astype(jnp.float32)).astype(jnp.bfloat16)
    return jnp.concatenate([high, low], axis=0)


def times(pair, factor):
    both = jnp.dot(pair, factor, preferred_element_type=jnp.float32)
    rows = both.shape[0] // 2
    return both[:rows] + both[rows:]


def pick_lanes(blocks, high, low):
    rows = blocks[0].shape[0]
    high = jnp.broadcast_to(high, (rows, LANES))
    low = jnp.broadcast_to(low, (rows, LANES))
    out = jnp.take_along_axis(blocks[0], low, axis=1)
    for b in range(1, len(blocks)):
        out = jnp.where(high == b, jnp.take_along_axis(blocks[b], low, axis=1), out)
    return out


def column_blocks(x, leaves):
    return [x[:, b * LANES : (b + 1) * LANES].astype(jnp.float32) for b in range(leaves)]


def first_body(points, order, compress, block_map, sent, pts, idx, comp, table, slot, rank, sems):
    leaves = idx.shape[0]
    copies = [
        pltpu.make_async_copy(block_map, table, sems.at[0]),
        pltpu.make_async_copy(order, idx, sems.at[1]),
        pltpu.make_async_copy(points, pts, sems.at[2]),
        pltpu.make_async_copy(compress, comp, sems.at[3]),
    ]
    for copy in copies:
        copy.start()
    copies[0].wait()
    tables(table, 0, slot, rank, leaves)
    copies[1].wait()
    copies[2].wait()
    blocks = column_blocks(pts[...], leaves)
    rows = []
    for k in range(leaves // 2):
        local = idx[pl.ds(slot[k], 1), :] & (leaves * LANES - 1)
        rows.append(pick_lanes(blocks, local >> 7, local & (LANES - 1)).astype(jnp.bfloat16))
    copies[3].wait()
    for k in range(leaves // 2):
        sent[k] = split(jnp.dot(rows[k], comp[slot[k]], preferred_element_type=jnp.float32))


def order_body(
    places, points, order, block_map, near, mixers, dense, expand,
    ordered, even, odd, table, mixers_out, dense_out, expand_out, maps, nears, slot, rank, sems,
):
    leaves = order.shape[0]
    levels = maps.shape[0]
    copies = [
        pltpu.make_async_copy(block_map, maps, sems.at[0]),
        pltpu.make_async_copy(near, nears, sems.at[1]),
        pltpu.make_async_copy(mixers, mixers_out, sems.at[2]),
        pltpu.make_async_copy(dense, dense_out, sems.at[3]),
        pltpu.make_async_copy(expand, expand_out, sems.at[4]),
    ]
    for copy in copies:
        copy.start()
    blocks = column_blocks(points[...], leaves)
    for leaf in range(leaves):
        local = order[pl.ds(leaf, 1), :] & (leaves * LANES - 1)
        ordered[leaf] = pick_lanes(blocks, local >> 7, local & (LANES - 1)).astype(jnp.bfloat16)
    block = lax.axis_index("block")
    parity = block & 1
    head, tail = 0, leaves - REACH
    even[...] = ordered[pl.ds(jnp.where(parity == 0, tail, head), REACH)]
    odd[...] = ordered[pl.ds(jnp.where(parity == 0, head, tail), REACH)]
    base = (lax.axis_index("partner") * lax.axis_size("block") + block) * leaves

    def put(row, value):
        table[pl.ds(row, 1), :] = jnp.full((1, LANES), value, jnp.int32)

    copies[0].wait()
    copies[1].wait()
    for level in range(levels):
        tables(maps, level, slot, rank, leaves)
        for i in range(leaves):
            put(places.piece(level, i), rank[maps[level, i]])
        if level > 0:
            for k in range(leaves // 2):
                i = slot[k]
                put(places.slot(level, k), i)
                put(places.slot_piece(level, k), read(table, places.piece(level - 1, i)))
    for leaf in range(leaves):
        for n in range(nears.shape[0]):
            put(places.near(leaf, n), nears[n, leaf] - base + REACH)
    for copy in copies[2:]:
        copy.wait()


def near_body(
    places, table, even, ordered, odd, blocks, order, mixers, expand, field, place, joint_own, joint, windows
):
    leaves, near_count = blocks.shape[0], blocks.shape[1]
    parity = lax.axis_index("block") & 1
    first, last = 0, leaves + REACH
    windows[pl.ds(jnp.where(parity == 0, last, first), REACH)] = even[...]
    windows[pl.ds(jnp.where(parity == 0, first, last), REACH)] = odd[...]
    windows[pl.ds(REACH, leaves)] = ordered[...]
    for leaf in range(leaves):
        total = None
        for n in range(near_count):
            source = windows[read(table, places.near(leaf, n))]
            term = jnp.dot(source, blocks[leaf, n], preferred_element_type=jnp.float32)
            total = term if total is None else total + term
        field[leaf] = total
    count = leaves * LANES
    target = lax.broadcasted_iota(jnp.int32, (count, LANES), 0)
    kind = lax.broadcasted_iota(jnp.int32, (8, LANES), 0)
    lane = lax.broadcasted_iota(jnp.int32, (8, LANES), 1)
    total = None
    for leaf in range(leaves):
        local = order[pl.ds(leaf, 1), :] & (count - 1)
        hit = jnp.where(target == local, 1.0, 0.0).astype(jnp.bfloat16)
        value = jnp.where(kind == 0, leaf, lane).astype(jnp.float32).astype(jnp.bfloat16)
        term = lax.dot_general(
            value, hit, (((1,), (1,)), ((), ())), preferred_element_type=jnp.float32
        )
        total = term if total is None else total + term
    place[...] = total.astype(jnp.int32)
    for side, out in enumerate((joint_own, joint)):
        for i in range(leaves):
            both = jnp.dot(
                mixers[mixers.shape[0] - 1, i, side], expand[i], preferred_element_type=jnp.float32
            )
            high = both.astype(jnp.bfloat16)
            out[i, :, :LANES] = high
            out[i, :, LANES:] = (both - high.astype(jnp.float32)).astype(jnp.bfloat16)


def top_send_body(places, table, received, factor, sent):
    for k in range(sent.shape[0]):
        i = read(table, places.slot(1, k))
        sent[k] = split(times(received[read(table, places.slot_piece(1, k))], factor[i]))


def top_own_body(places, table, received, factor, mixers, own):
    for i in range(own.shape[0]):
        state = split(times(received[read(table, places.piece(0, i))], factor[i]))
        own[i] = times(state, mixers[0, i, 0])


def mix_send_body(places, level, table, received, own, mixers, sent):
    for k in range(sent.shape[0]):
        i = read(table, places.slot(level + 1, k))
        piece = received[read(table, places.slot_piece(level + 1, k))]
        sent[k] = split(own[i] + times(piece, mixers[level - 1, i, 1]))


def mix_own_body(places, level, table, received, own, mixers, own_next):
    for i in range(own.shape[0]):
        other = times(received[read(table, places.piece(level, i))], mixers[level - 1, i, 1])
        own_next[i] = times(split(own[i] + other), mixers[level, i, 0])


def times_joint(pair, joint):
    both = jnp.dot(pair, joint, preferred_element_type=jnp.float32)
    rows = both.shape[0] // 2
    return (both[:rows, :LANES] + both[rows:, :LANES]) + (both[:rows, LANES:] + both[rows:, LANES:])


def base_body(places, level, table, received, own, mixers, joint_own, field, base):
    for i in range(own.shape[0]):
        other = times(received[read(table, places.piece(level, i))], mixers[level - 1, i, 1])
        base[i] = field[i] + times_joint(split(own[i] + other), joint_own[i])


def last_body(places, level, table, received, base, joint, place, applied, rows, sems):
    leaves = base.shape[0]
    blocks = []
    for i in range(leaves):
        piece = received[read(table, places.piece(level, i))]
        blocks.append((base[i] + times_joint(piece, joint[i])).astype(jnp.bfloat16).astype(jnp.float32))
    group = rows.shape[0] // sems.shape[0]
    copies = []
    for g in range(sems.shape[0]):
        here = slice(g * group, (g + 1) * group)
        part = [block[here] for block in blocks]
        for b in range(leaves):
            lanes = slice(b * LANES, (b + 1) * LANES)
            picked = pick_lanes(part, place[pl.ds(0, 1), lanes], place[pl.ds(1, 1), lanes])
            rows[here, lanes] = picked.astype(jnp.bfloat16)
        copies.append(pltpu.make_async_copy(rows.at[here], applied.at[here], sems.at[g]))
        copies[-1].start()
    for copy in copies:
        copy.wait()


def from_partner(x, bit):
    count = lax.axis_size("partner")
    return lax.ppermute(x, "partner", [(i, i ^ 1 << bit) for i in range(count)])


def with_neighbour(x, first):
    groups, count = lax.axis_size("partner"), lax.axis_size("block")
    to = {}
    for g in range(groups):
        for i in range(count):
            to[g * count + i] = (g ^ 1) * count + i
        for i in range(first, count - 1, 2):
            to[g * count + i], to[g * count + i + 1] = g * count + i + 1, g * count + i
    return lax.ppermute(x, ("partner", "block"), sorted(to.items()))


def on_device(
    points,
    tree_order,
    nearby_dense_blocks,
    neighbours,
    compress,
    expand,
    top_factor,
    butterfly_mixers,
    block_map,
):
    vectors, count = points.shape
    leaves, near_count = neighbours.shape
    levels = lax.axis_size("partner").bit_length() - 1
    half = leaves // 2
    places = Places(levels, leaves, near_count)
    order = tree_order.reshape(leaves, LANES)
    ints = pltpu.SMEM((leaves + 1,), jnp.int32)
    pair = jax.ShapeDtypeStruct((half, 2 * vectors, LANES), jnp.bfloat16)
    state = jax.ShapeDtypeStruct((leaves, vectors, LANES), jnp.float32)
    edge = jax.ShapeDtypeStruct((REACH, vectors, LANES), jnp.bfloat16)
    part = functools.partial
    assert levels > 2

    sent = call(
        first_body,
        pair,
        [HBM, HBM, HBM, HBM],
        [
            pltpu.VMEM(points.shape, points.dtype),
            pltpu.VMEM(order.shape, order.dtype),
            pltpu.VMEM(compress.shape, compress.dtype),
            pltpu.SMEM(block_map.shape, block_map.dtype),
            ints,
            ints,
            pltpu.SemaphoreType.DMA((4,)),
        ],
    )(points, order, compress, block_map)
    received = from_partner(sent, levels - 1)

    ordered, even, odd, table, mixers, dense, expand = call(
        part(order_body, places),
        [
            jax.ShapeDtypeStruct((leaves, vectors, LANES), jnp.bfloat16),
            edge,
            edge,
            jax.ShapeDtypeStruct((places.rows, LANES), jnp.int32),
            jax.ShapeDtypeStruct(butterfly_mixers.shape, butterfly_mixers.dtype),
            jax.ShapeDtypeStruct(nearby_dense_blocks.shape, nearby_dense_blocks.dtype),
            jax.ShapeDtypeStruct(expand.shape, expand.dtype),
        ],
        [VMEM, VMEM, HBM, HBM, HBM, HBM, HBM],
        [
            pltpu.SMEM(block_map.shape, block_map.dtype),
            pltpu.SMEM((near_count, leaves), neighbours.dtype),
            ints,
            ints,
            pltpu.SemaphoreType.DMA((5,)),
        ],
        flops=1 << 24,
    )(points, order, block_map, neighbours.T, butterfly_mixers, nearby_dense_blocks, expand)
    even = with_neighbour(even, 0)
    odd = with_neighbour(odd, 1)

    sent = call(part(top_send_body, places), pair, [VMEM] * 3)(table, received, top_factor)
    own = call(part(top_own_body, places), state, [VMEM] * 4, flops=1 << 24)(
        table, received, top_factor, mixers
    )
    wide = jax.ShapeDtypeStruct((leaves, LANES, 2 * LANES), jnp.bfloat16)
    field, place, joint_own, joint = call(
        part(near_body, places),
        [
            state,
            jax.ShapeDtypeStruct((8, count), jnp.int32),
            wide,
            wide,
        ],
        [VMEM] * 8,
        [pltpu.VMEM((leaves + 2 * REACH, vectors, LANES), jnp.bfloat16)],
        flops=1 << 25,
    )(table, even, ordered, odd, dense, order, mixers, expand)

    for level in range(1, levels):
        received = from_partner(sent, levels - 1 - level)
        if level < levels - 1:
            sent = call(part(mix_send_body, places, level), pair, [VMEM] * 4)(
                table, received, own, mixers
            )
            if level < levels - 2:
                body, factors = mix_own_body, (mixers,)
            else:
                body, factors = base_body, (mixers, joint_own, field)
            own = call(
                part(body, places, level), state, [VMEM] * (3 + len(factors)), flops=1 << 24
            )(table, received, own, *factors)
    return call(
        part(last_body, places, levels - 1),
        jax.ShapeDtypeStruct(points.shape, points.dtype),
        [VMEM] * 5,
        [pltpu.VMEM(points.shape, points.dtype), pltpu.SemaphoreType.DMA((4,))],
        place=HBM,
    )(table, received, own, joint, place)


def solution(mesh):
    return jax.shard_map(
        on_device,
        mesh=mesh,
        in_specs=(
            P(None, ("partner", "block")),
            P(("partner", "block")),
            P(("partner", "block"), None, None, None),
            P(("partner", "block"), None),
            P(("partner", "block"), None, None),
            P(("partner", "block"), None, None),
            P(("partner", "block"), None, None),
            P(None, ("partner", "block"), None, None, None),
            P(),
        ),
        out_specs=P(None, ("partner", "block")),
        check_vma=False,
    )
```

```python
import functools

import jax
import jax.numpy as jnp
from jax import lax
from jax.experimental import pallas as pl
from jax.experimental.pallas import tpu as pltpu
from jax.sharding import PartitionSpec as P


REACH = 2
LANES = 128
VMEM = pl.BlockSpec(memory_space=pltpu.VMEM)
HBM = pl.BlockSpec(memory_space=pltpu.HBM)


def call(body, outs, in_specs, scratch=(), flops=1 << 20, moved=1 << 18, place=VMEM):
    single = not isinstance(outs, (list, tuple))
    run = pl.pallas_call(
        body,
        out_shape=outs,
        in_specs=in_specs,
        out_specs=place if single else [VMEM] * len(outs),
        scratch_shapes=list(scratch),
        compiler_params=pltpu.CompilerParams(vmem_limit_bytes=16 << 20),
        cost_estimate=pl.CostEstimate(flops=flops, bytes_accessed=moved, transcendentals=0),
    )

    def bound(*args):
        return run(
            *[
                pltpu.with_memory_space_constraint(a, pltpu.HBM) if s is HBM else a
                for a, s in zip(args, in_specs)
            ]
        )

    return bound


def tables(map_ref, row, slot_ref, rank_ref, slots):
    mask = jnp.int32(0)
    for i in range(slots):
        mask = mask | (jnp.int32(1) << map_ref[row, i])
    rank = jnp.int32(0)
    for j in range(slots):
        slot_ref[rank] = jnp.int32(j)
        rank_ref[j] = rank
        rank = rank + ((mask >> j) & 1)


class Places:
    def __init__(self, levels, leaves, near_count):
        self.leaves, self.half = leaves, leaves // 2
        self.level_rows = leaves + 2 * self.half
        self.near_base = levels * self.level_rows
        self.near_count = near_count
        self.rows = -(-(self.near_base + leaves * near_count) // 8) * 8

    def piece(self, level, i):
        return level * self.level_rows + i

    def slot(self, level, k):
        return level * self.level_rows + self.leaves + k

    def slot_piece(self, level, k):
        return level * self.level_rows + self.leaves + self.half + k

    def near(self, leaf, n):
        return self.near_base + leaf * self.near_count + n


def read(table, row):
    return table[pl.ds(row, 1), :][0, 0]


def split(x):
    high = x.astype(jnp.bfloat16)
    low = (x - high.astype(jnp.float32)).astype(jnp.bfloat16)
    return jnp.concatenate([high, low], axis=0)


def times(pair, factor):
    both = jnp.dot(pair, factor, preferred_element_type=jnp.float32)
    rows = both.shape[0] // 2
    return both[:rows] + both[rows:]


def pick_lanes(blocks, high, low):
    rows = blocks[0].shape[0]
    high = jnp.broadcast_to(high, (rows, LANES))
    low = jnp.broadcast_to(low, (rows, LANES))
    out = jnp.take_along_axis(blocks[0], low, axis=1)
    for b in range(1, len(blocks)):
        out = jnp.where(high == b, jnp.take_along_axis(blocks[b], low, axis=1), out)
    return out


def column_blocks(x, leaves):
    return [x[:, b * LANES : (b + 1) * LANES].astype(jnp.float32) for b in range(leaves)]


def first_body(points, order, compress, block_map, sent, pts, idx, comp, table, slot, rank, sems):
    leaves = idx.shape[0]
    copies = [
        pltpu.make_async_copy(block_map, table, sems.at[0]),
        pltpu.make_async_copy(order, idx, sems.at[1]),
        pltpu.make_async_copy(points, pts, sems.at[2]),
        pltpu.make_async_copy(compress, comp, sems.at[3]),
    ]
    for copy in copies:
        copy.start()
    copies[0].wait()
    tables(table, 0, slot, rank, leaves)
    copies[1].wait()
    copies[2].wait()
    blocks = column_blocks(pts[...], leaves)
    rows = []
    for k in range(leaves // 2):
        local = idx[pl.ds(slot[k], 1), :] & (leaves * LANES - 1)
        rows.append(pick_lanes(blocks, local >> 7, local & (LANES - 1)).astype(jnp.bfloat16))
    copies[3].wait()
    for k in range(leaves // 2):
        sent[k] = split(jnp.dot(rows[k], comp[slot[k]], preferred_element_type=jnp.float32))


def order_body(
    places, points, order, block_map, near, mixers, dense, expand,
    ordered, even, odd, table, mixers_out, dense_out, expand_out, maps, nears, slot, rank, sems,
):
    leaves = order.shape[0]
    levels = maps.shape[0]
    copies = [
        pltpu.make_async_copy(block_map, maps, sems.at[0]),
        pltpu.make_async_copy(near, nears, sems.at[1]),
        pltpu.make_async_copy(mixers, mixers_out, sems.at[2]),
        pltpu.make_async_copy(dense, dense_out, sems.at[3]),
        pltpu.make_async_copy(expand, expand_out, sems.at[4]),
    ]
    for copy in copies:
        copy.start()
    blocks = column_blocks(points[...], leaves)
    for leaf in range(leaves):
        local = order[pl.ds(leaf, 1), :] & (leaves * LANES - 1)
        ordered[leaf] = pick_lanes(blocks, local >> 7, local & (LANES - 1)).astype(jnp.bfloat16)
    block = lax.axis_index("block")
    parity = block & 1
    head, tail = 0, leaves - REACH
    even[...] = ordered[pl.ds(jnp.where(parity == 0, tail, head), REACH)]
    odd[...] = ordered[pl.ds(jnp.where(parity == 0, head, tail), REACH)]
    base = (lax.axis_index("partner") * lax.axis_size("block") + block) * leaves

    def put(row, value):
        table[pl.ds(row, 1), :] = jnp.full((1, LANES), value, jnp.int32)

    copies[0].wait()
    copies[1].wait()
    for level in range(levels):
        tables(maps, level, slot, rank, leaves)
        for i in range(leaves):
            put(places.piece(level, i), rank[maps[level, i]])
        if level > 0:
            for k in range(leaves // 2):
                i = slot[k]
                put(places.slot(level, k), i)
                put(places.slot_piece(level, k), read(table, places.piece(level - 1, i)))
    for leaf in range(leaves):
        for n in range(nears.shape[0]):
            put(places.near(leaf, n), nears[n, leaf] - base + REACH)
    for copy in copies[2:]:
        copy.wait()


def prep_body(order, mixers, expand, place, joint_own, joint):
    leaves = order.shape[0]
    count = leaves * LANES
    target = lax.broadcasted_iota(jnp.int32, (count, LANES), 0)
    kind = lax.broadcasted_iota(jnp.int32, (8, LANES), 0)
    lane = lax.broadcasted_iota(jnp.int32, (8, LANES), 1)
    total = None
    for leaf in range(leaves):
        local = order[pl.ds(leaf, 1), :] & (count - 1)
        hit = jnp.where(target == local, 1.0, 0.0).astype(jnp.bfloat16)
        value = jnp.where(kind == 0, leaf, lane).astype(jnp.float32).astype(jnp.bfloat16)
        term = lax.dot_general(
            value, hit, (((1,), (1,)), ((), ())), preferred_element_type=jnp.float32
        )
        total = term if total is None else total + term
    place[...] = total.astype(jnp.int32)
    for side, out in enumerate((joint_own, joint)):
        for i in range(leaves):
            both = jnp.dot(
                mixers[mixers.shape[0] - 1, i, side], expand[i], preferred_element_type=jnp.float32
            )
            high = both.astype(jnp.bfloat16)
            out[i, :, :LANES] = high
            out[i, :, LANES:] = (both - high.astype(jnp.float32)).astype(jnp.bfloat16)


def top_send_body(places, table, received, factor, sent):
    for k in range(sent.shape[0]):
        i = read(table, places.slot(1, k))
        sent[k] = split(times(received[read(table, places.slot_piece(1, k))], factor[i]))


def top_own_body(places, table, received, factor, mixers, own):
    for i in range(own.shape[0]):
        state = split(times(received[read(table, places.piece(0, i))], factor[i]))
        own[i] = times(state, mixers[0, i, 0])


def mix_send_body(places, level, table, received, own, mixers, sent):
    for k in range(sent.shape[0]):
        i = read(table, places.slot(level + 1, k))
        piece = received[read(table, places.slot_piece(level + 1, k))]
        sent[k] = split(own[i] + times(piece, mixers[level - 1, i, 1]))


def mix_own_body(places, level, table, received, own, mixers, own_next):
    for i in range(own.shape[0]):
        other = times(received[read(table, places.piece(level, i))], mixers[level - 1, i, 1])
        own_next[i] = times(split(own[i] + other), mixers[level, i, 0])


def times_joint(pair, joint):
    both = jnp.dot(pair, joint, preferred_element_type=jnp.float32)
    rows = both.shape[0] // 2
    return (both[:rows, :LANES] + both[rows:, :LANES]) + (both[:rows, LANES:] + both[rows:, LANES:])


def base_body(
    places, level, table, received, own, mixers, joint_own, even, ordered, odd, dense, base, windows
):
    leaves, near_count = dense.shape[0], dense.shape[1]
    parity = lax.axis_index("block") & 1
    first, last = 0, leaves + REACH
    windows[pl.ds(jnp.where(parity == 0, last, first), REACH)] = even[...]
    windows[pl.ds(jnp.where(parity == 0, first, last), REACH)] = odd[...]
    windows[pl.ds(REACH, leaves)] = ordered[...]
    for i in range(leaves):
        other = times(received[read(table, places.piece(level, i))], mixers[level - 1, i, 1])
        total = times_joint(split(own[i] + other), joint_own[i])
        for n in range(near_count):
            source = windows[read(table, places.near(i, n))]
            total = total + jnp.dot(source, dense[i, n], preferred_element_type=jnp.float32)
        base[i] = total


def last_body(places, level, table, received, base, joint, place, applied, rows, sems):
    leaves = base.shape[0]
    blocks = []
    for i in range(leaves):
        piece = received[read(table, places.piece(level, i))]
        blocks.append((base[i] + times_joint(piece, joint[i])).astype(jnp.bfloat16).astype(jnp.float32))
    group = rows.shape[0] // sems.shape[0]
    copies = []
    for g in range(sems.shape[0]):
        here = slice(g * group, (g + 1) * group)
        part = [block[here] for block in blocks]
        for b in range(leaves):
            lanes = slice(b * LANES, (b + 1) * LANES)
            picked = pick_lanes(part, place[pl.ds(0, 1), lanes], place[pl.ds(1, 1), lanes])
            rows[here, lanes] = picked.astype(jnp.bfloat16)
        copies.append(pltpu.make_async_copy(rows.at[here], applied.at[here], sems.at[g]))
        copies[-1].start()
    for copy in copies:
        copy.wait()


def from_partner(x, bit):
    count = lax.axis_size("partner")
    return lax.ppermute(x, "partner", [(i, i ^ 1 << bit) for i in range(count)])


def with_neighbour(x, first):
    groups, count = lax.axis_size("partner"), lax.axis_size("block")
    to = {}
    for g in range(groups):
        for i in range(count):
            to[g * count + i] = (g ^ 1) * count + i
        for i in range(first, count - 1, 2):
            to[g * count + i], to[g * count + i + 1] = g * count + i + 1, g * count + i
    return lax.ppermute(x, ("partner", "block"), sorted(to.items()))


def on_device(
    points,
    tree_order,
    nearby_dense_blocks,
    neighbours,
    compress,
    expand,
    top_factor,
    butterfly_mixers,
    block_map,
):
    vectors, count = points.shape
    leaves, near_count = neighbours.shape
    levels = lax.axis_size("partner").bit_length() - 1
    half = leaves // 2
    places = Places(levels, leaves, near_count)
    order = tree_order.reshape(leaves, LANES)
    ints = pltpu.SMEM((leaves + 1,), jnp.int32)
    pair = jax.ShapeDtypeStruct((half, 2 * vectors, LANES), jnp.bfloat16)
    state = jax.ShapeDtypeStruct((leaves, vectors, LANES), jnp.float32)
    edge = jax.ShapeDtypeStruct((REACH, vectors, LANES), jnp.bfloat16)
    part = functools.partial
    assert levels > 2

    sent = call(
        first_body,
        pair,
        [HBM, HBM, HBM, HBM],
        [
            pltpu.VMEM(points.shape, points.dtype),
            pltpu.VMEM(order.shape, order.dtype),
            pltpu.VMEM(compress.shape, compress.dtype),
            pltpu.SMEM(block_map.shape, block_map.dtype),
            ints,
            ints,
            pltpu.SemaphoreType.DMA((4,)),
        ],
    )(points, order, compress, block_map)
    received = from_partner(sent, levels - 1)

    ordered, even, odd, table, mixers, dense, expand = call(
        part(order_body, places),
        [
            jax.ShapeDtypeStruct((leaves, vectors, LANES), jnp.bfloat16),
            edge,
            edge,
            jax.ShapeDtypeStruct((places.rows, LANES), jnp.int32),
            jax.ShapeDtypeStruct(butterfly_mixers.shape, butterfly_mixers.dtype),
            jax.ShapeDtypeStruct(nearby_dense_blocks.shape, nearby_dense_blocks.dtype),
            jax.ShapeDtypeStruct(expand.shape, expand.dtype),
        ],
        [VMEM, VMEM, HBM, HBM, HBM, HBM, HBM],
        [
            pltpu.SMEM(block_map.shape, block_map.dtype),
            pltpu.SMEM((near_count, leaves), neighbours.dtype),
            ints,
            ints,
            pltpu.SemaphoreType.DMA((5,)),
        ],
        flops=1 << 24,
    )(points, order, block_map, neighbours.T, butterfly_mixers, nearby_dense_blocks, expand)
    even = with_neighbour(even, 0)
    odd = with_neighbour(odd, 1)

    sent = call(part(top_send_body, places), pair, [VMEM] * 3)(table, received, top_factor)
    own = call(part(top_own_body, places), state, [VMEM] * 4, flops=1 << 24)(
        table, received, top_factor, mixers
    )
    wide = jax.ShapeDtypeStruct((leaves, LANES, 2 * LANES), jnp.bfloat16)
    place, joint_own, joint = call(
        prep_body,
        [jax.ShapeDtypeStruct((8, count), jnp.int32), wide, wide],
        [VMEM] * 3,
        flops=1 << 24,
    )(order, mixers, expand)

    for level in range(1, levels):
        received = from_partner(sent, levels - 1 - level)
        if level < levels - 1:
            sent = call(part(mix_send_body, places, level), pair, [VMEM] * 4)(
                table, received, own, mixers
            )
            if level < levels - 2:
                body, factors, scratch = mix_own_body, (mixers,), ()
            else:
                body = base_body
                factors = (mixers, joint_own, even, ordered, odd, dense)
                scratch = [pltpu.VMEM((leaves + 2 * REACH, vectors, LANES), jnp.bfloat16)]
            own = call(
                part(body, places, level),
                state,
                [VMEM] * (3 + len(factors)),
                scratch,
                flops=1 << 24,
            )(table, received, own, *factors)
    return call(
        part(last_body, places, levels - 1),
        jax.ShapeDtypeStruct(points.shape, points.dtype),
        [VMEM] * 5,
        [pltpu.VMEM(points.shape, points.dtype), pltpu.SemaphoreType.DMA((2,))],
        place=HBM,
    )(table, received, own, joint, place)


def solution(mesh):
    return jax.shard_map(
        on_device,
        mesh=mesh,
        in_specs=(
            P(None, ("partner", "block")),
            P(("partner", "block")),
            P(("partner", "block"), None, None, None),
            P(("partner", "block"), None),
            P(("partner", "block"), None, None),
            P(("partner", "block"), None, None),
            P(("partner", "block"), None, None),
            P(None, ("partner", "block"), None, None, None),
            P(),
        ),
        out_specs=P(None, ("partner", "block")),
        check_vma=False,
    )
```

```python
import functools

import jax
import jax.numpy as jnp
from jax import lax
from jax.experimental import pallas as pl
from jax.experimental.pallas import tpu as pltpu
from jax.sharding import PartitionSpec as P


REACH = 2
LANES = 128
VMEM = pl.BlockSpec(memory_space=pltpu.VMEM)
HBM = pl.BlockSpec(memory_space=pltpu.HBM)


def call(body, outs, in_specs, scratch=(), flops=1 << 20, moved=1 << 18, place=VMEM):
    single = not isinstance(outs, (list, tuple))
    run = pl.pallas_call(
        body,
        out_shape=outs,
        in_specs=in_specs,
        out_specs=place if single else [VMEM] * len(outs),
        scratch_shapes=list(scratch),
        compiler_params=pltpu.CompilerParams(vmem_limit_bytes=16 << 20),
        cost_estimate=pl.CostEstimate(flops=flops, bytes_accessed=moved, transcendentals=0),
    )

    def bound(*args):
        return run(
            *[
                pltpu.with_memory_space_constraint(a, pltpu.HBM) if s is HBM else a
                for a, s in zip(args, in_specs)
            ]
        )

    return bound


def tables(map_ref, row, slot_ref, rank_ref, slots):
    mask = jnp.int32(0)
    for i in range(slots):
        mask = mask | (jnp.int32(1) << map_ref[row, i])
    rank = jnp.int32(0)
    for j in range(slots):
        slot_ref[rank] = jnp.int32(j)
        rank_ref[j] = rank
        rank = rank + ((mask >> j) & 1)


class Places:
    def __init__(self, levels, leaves, near_count):
        self.leaves, self.half = leaves, leaves // 2
        self.level_rows = leaves + 2 * self.half
        self.near_base = levels * self.level_rows
        self.near_count = near_count
        self.rows = -(-(self.near_base + leaves * near_count) // 8) * 8

    def piece(self, level, i):
        return level * self.level_rows + i

    def slot(self, level, k):
        return level * self.level_rows + self.leaves + k

    def slot_piece(self, level, k):
        return level * self.level_rows + self.leaves + self.half + k

    def near(self, leaf, n):
        return self.near_base + leaf * self.near_count + n


def read(table, row):
    return table[pl.ds(row, 1), :][0, 0]


def split(x):
    high = x.astype(jnp.bfloat16)
    low = (x - high.astype(jnp.float32)).astype(jnp.bfloat16)
    return jnp.concatenate([high, low], axis=0)


def times(pair, factor):
    both = jnp.dot(pair, factor, preferred_element_type=jnp.float32)
    rows = both.shape[0] // 2
    return both[:rows] + both[rows:]


def pick_lanes(blocks, high, low):
    rows = blocks[0].shape[0]
    high = jnp.broadcast_to(high, (rows, LANES))
    low = jnp.broadcast_to(low, (rows, LANES))
    out = jnp.take_along_axis(blocks[0], low, axis=1)
    for b in range(1, len(blocks)):
        out = jnp.where(high == b, jnp.take_along_axis(blocks[b], low, axis=1), out)
    return out


def column_blocks(x, leaves):
    return [x[:, b * LANES : (b + 1) * LANES].astype(jnp.float32) for b in range(leaves)]


def first_body(
    places, points, order, compress, block_map, near,
    sent, table, pts, idx, comp, maps, nears, slots, ranks, sems,
):
    leaves = idx.shape[0]
    levels = maps.shape[0]
    copies = [
        pltpu.make_async_copy(block_map, maps, sems.at[0]),
        pltpu.make_async_copy(near, nears, sems.at[1]),
        pltpu.make_async_copy(order, idx, sems.at[2]),
        pltpu.make_async_copy(points, pts, sems.at[3]),
        pltpu.make_async_copy(compress, comp, sems.at[4]),
    ]
    for copy in copies:
        copy.start()

    def put(row, value):
        table[pl.ds(row, 1), :] = jnp.full((1, LANES), value, jnp.int32)

    copies[0].wait()
    for level in range(levels):
        slot, rank = slots.at[level], ranks.at[level]
        tables(maps, level, slot, rank, leaves)
        for i in range(leaves):
            put(places.piece(level, i), rank[maps[level, i]])
        if level > 0:
            for k in range(leaves // 2):
                i = slot[k]
                put(places.slot(level, k), i)
                put(places.slot_piece(level, k), ranks[level - 1, maps[level - 1, i]])
    copies[1].wait()
    device = lax.axis_index("partner") * lax.axis_size("block") + lax.axis_index("block")
    base = device * leaves
    for leaf in range(leaves):
        for n in range(nears.shape[0]):
            put(places.near(leaf, n), nears[n, leaf] - base + REACH)
    copies[2].wait()
    copies[3].wait()
    blocks = column_blocks(pts[...], leaves)
    rows = []
    for k in range(leaves // 2):
        local = idx[pl.ds(slots[0, k], 1), :] & (leaves * LANES - 1)
        rows.append(pick_lanes(blocks, local >> 7, local & (LANES - 1)).astype(jnp.bfloat16))
    copies[4].wait()
    for k in range(leaves // 2):
        product = jnp.dot(rows[k], comp[slots[0, k]], preferred_element_type=jnp.float32)
        sent[k] = split(product)


def order_body(points, order, ordered, even, odd):
    leaves = order.shape[0]
    blocks = column_blocks(points[...], leaves)
    for leaf in range(leaves):
        local = order[pl.ds(leaf, 1), :] & (leaves * LANES - 1)
        ordered[leaf] = pick_lanes(blocks, local >> 7, local & (LANES - 1)).astype(jnp.bfloat16)
    parity = lax.axis_index("block") & 1
    head, tail = 0, leaves - REACH
    even[...] = ordered[pl.ds(jnp.where(parity == 0, tail, head), REACH)]
    odd[...] = ordered[pl.ds(jnp.where(parity == 0, head, tail), REACH)]


def prep_body(
    order, mixers_in, dense_in, expand_in, place, joint_own, joint, mixers, dense, expand, sems
):
    leaves = order.shape[0]
    copies = [
        pltpu.make_async_copy(expand_in, expand, sems.at[0]),
        pltpu.make_async_copy(mixers_in, mixers, sems.at[1]),
        pltpu.make_async_copy(dense_in, dense, sems.at[2]),
    ]
    for copy in copies:
        copy.start()
    count = leaves * LANES
    target = lax.broadcasted_iota(jnp.int32, (count, LANES), 0)
    kind = lax.broadcasted_iota(jnp.int32, (8, LANES), 0)
    lane = lax.broadcasted_iota(jnp.int32, (8, LANES), 1)
    total = None
    for leaf in range(leaves):
        local = order[pl.ds(leaf, 1), :] & (count - 1)
        hit = jnp.where(target == local, 1.0, 0.0).astype(jnp.bfloat16)
        value = jnp.where(kind == 0, leaf, lane).astype(jnp.float32).astype(jnp.bfloat16)
        term = lax.dot_general(
            value, hit, (((1,), (1,)), ((), ())), preferred_element_type=jnp.float32
        )
        total = term if total is None else total + term
    place[...] = total.astype(jnp.int32)
    copies[0].wait()
    copies[1].wait()
    for side, out in enumerate((joint_own, joint)):
        for i in range(leaves):
            both = jnp.dot(
                mixers[mixers.shape[0] - 1, i, side], expand[i], preferred_element_type=jnp.float32
            )
            high = both.astype(jnp.bfloat16)
            out[i, :, :LANES] = high
            out[i, :, LANES:] = (both - high.astype(jnp.float32)).astype(jnp.bfloat16)
    copies[2].wait()


def top_send_body(places, table, received, factor, sent):
    for k in range(sent.shape[0]):
        i = read(table, places.slot(1, k))
        sent[k] = split(times(received[read(table, places.slot_piece(1, k))], factor[i]))


def top_own_body(places, table, received, factor, mixers, own):
    for i in range(own.shape[0]):
        state = split(times(received[read(table, places.piece(0, i))], factor[i]))
        own[i] = times(state, mixers[0, i, 0])


def mix_send_body(places, level, table, received, own, mixers, sent):
    for k in range(sent.shape[0]):
        i = read(table, places.slot(level + 1, k))
        piece = received[read(table, places.slot_piece(level + 1, k))]
        sent[k] = split(own[i] + times(piece, mixers[level - 1, i, 1]))


def mix_own_body(places, level, table, received, own, mixers, own_next):
    for i in range(own.shape[0]):
        other = times(received[read(table, places.piece(level, i))], mixers[level - 1, i, 1])
        own_next[i] = times(split(own[i] + other), mixers[level, i, 0])


def times_joint(pair, joint):
    both = jnp.dot(pair, joint, preferred_element_type=jnp.float32)
    rows = both.shape[0] // 2
    return (both[:rows, :LANES] + both[rows:, :LANES]) + (both[:rows, LANES:] + both[rows:, LANES:])


def base_body(
    places, level, table, received, own, mixers, joint_own, even, ordered, odd, dense, base, windows
):
    leaves, near_count = dense.shape[0], dense.shape[1]
    parity = lax.axis_index("block") & 1
    first, last = 0, leaves + REACH
    windows[pl.ds(jnp.where(parity == 0, last, first), REACH)] = even[...]
    windows[pl.ds(jnp.where(parity == 0, first, last), REACH)] = odd[...]
    windows[pl.ds(REACH, leaves)] = ordered[...]
    for i in range(leaves):
        other = times(received[read(table, places.piece(level, i))], mixers[level - 1, i, 1])
        total = times_joint(split(own[i] + other), joint_own[i])
        for n in range(near_count):
            source = windows[read(table, places.near(i, n))]
            total = total + jnp.dot(source, dense[i, n], preferred_element_type=jnp.float32)
        base[i] = total


def last_body(places, level, table, received, base, joint, place, applied, rows, sems):
    leaves = base.shape[0]
    blocks = []
    for i in range(leaves):
        piece = received[read(table, places.piece(level, i))]
        blocks.append((base[i] + times_joint(piece, joint[i])).astype(jnp.bfloat16).astype(jnp.float32))
    group = rows.shape[0] // sems.shape[0]
    copies = []
    for g in range(sems.shape[0]):
        here = slice(g * group, (g + 1) * group)
        part = [block[here] for block in blocks]
        for b in range(leaves):
            lanes = slice(b * LANES, (b + 1) * LANES)
            picked = pick_lanes(part, place[pl.ds(0, 1), lanes], place[pl.ds(1, 1), lanes])
            rows[here, lanes] = picked.astype(jnp.bfloat16)
        copies.append(pltpu.make_async_copy(rows.at[here], applied.at[here], sems.at[g]))
        copies[-1].start()
    for copy in copies:
        copy.wait()


def from_partner(x, bit):
    count = lax.axis_size("partner")
    return lax.ppermute(x, "partner", [(i, i ^ 1 << bit) for i in range(count)])


def with_neighbour(x, first):
    groups, count = lax.axis_size("partner"), lax.axis_size("block")
    to = {}
    for g in range(groups):
        for i in range(count):
            to[g * count + i] = (g ^ 1) * count + i
        for i in range(first, count - 1, 2):
            to[g * count + i], to[g * count + i + 1] = g * count + i + 1, g * count + i
    return lax.ppermute(x, ("partner", "block"), sorted(to.items()))


def on_device(
    points,
    tree_order,
    nearby_dense_blocks,
    neighbours,
    compress,
    expand,
    top_factor,
    butterfly_mixers,
    block_map,
):
    vectors, count = points.shape
    leaves, near_count = neighbours.shape
    levels = lax.axis_size("partner").bit_length() - 1
    half = leaves // 2
    places = Places(levels, leaves, near_count)
    order = tree_order.reshape(leaves, LANES)
    ints = pltpu.SMEM((levels, leaves + 1), jnp.int32)
    pair = jax.ShapeDtypeStruct((half, 2 * vectors, LANES), jnp.bfloat16)
    state = jax.ShapeDtypeStruct((leaves, vectors, LANES), jnp.float32)
    edge = jax.ShapeDtypeStruct((REACH, vectors, LANES), jnp.bfloat16)
    part = functools.partial
    assert levels > 2

    sent, table = call(
        part(first_body, places),
        [pair, jax.ShapeDtypeStruct((places.rows, LANES), jnp.int32)],
        [HBM] * 5,
        [
            pltpu.VMEM(points.shape, points.dtype),
            pltpu.VMEM(order.shape, order.dtype),
            pltpu.VMEM(compress.shape, compress.dtype),
            pltpu.SMEM(block_map.shape, block_map.dtype),
            pltpu.SMEM((near_count, leaves), neighbours.dtype),
            ints,
            ints,
            pltpu.SemaphoreType.DMA((5,)),
        ],
    )(points, order, compress, block_map, neighbours.T)
    received = from_partner(sent, levels - 1)

    ordered, even, odd = call(
        order_body,
        [jax.ShapeDtypeStruct((leaves, vectors, LANES), jnp.bfloat16), edge, edge],
        [VMEM] * 2,
        flops=1 << 24,
    )(points, order)
    even = with_neighbour(even, 0)
    odd = with_neighbour(odd, 1)

    sent = call(part(top_send_body, places), pair, [VMEM] * 3)(table, received, top_factor)
    wide = jax.ShapeDtypeStruct((leaves, LANES, 2 * LANES), jnp.bfloat16)
    place, joint_own, joint, mixers, dense = call(
        prep_body,
        [
            jax.ShapeDtypeStruct((8, count), jnp.int32),
            wide,
            wide,
            jax.ShapeDtypeStruct(butterfly_mixers.shape, butterfly_mixers.dtype),
            jax.ShapeDtypeStruct(nearby_dense_blocks.shape, nearby_dense_blocks.dtype),
        ],
        [VMEM] + [HBM] * 3,
        [pltpu.VMEM(expand.shape, expand.dtype), pltpu.SemaphoreType.DMA((3,))],
        flops=1 << 24,
    )(order, butterfly_mixers, nearby_dense_blocks, expand)
    own = call(part(top_own_body, places), state, [VMEM] * 4, flops=1 << 24)(
        table, received, top_factor, mixers
    )

    for level in range(1, levels):
        received = from_partner(sent, levels - 1 - level)
        if level < levels - 1:
            sent = call(part(mix_send_body, places, level), pair, [VMEM] * 4)(
                table, received, own, mixers
            )
            if level < levels - 2:
                body, factors, scratch = mix_own_body, (mixers,), ()
            else:
                body = base_body
                factors = (mixers, joint_own, even, ordered, odd, dense)
                scratch = [pltpu.VMEM((leaves + 2 * REACH, vectors, LANES), jnp.bfloat16)]
            own = call(
                part(body, places, level),
                state,
                [VMEM] * (3 + len(factors)),
                scratch,
                flops=1 << 24,
            )(table, received, own, *factors)
    return call(
        part(last_body, places, levels - 1),
        jax.ShapeDtypeStruct(points.shape, points.dtype),
        [VMEM] * 5,
        [pltpu.VMEM(points.shape, points.dtype), pltpu.SemaphoreType.DMA((2,))],
        place=HBM,
    )(table, received, own, joint, place)


def solution(mesh):
    return jax.shard_map(
        on_device,
        mesh=mesh,
        in_specs=(
            P(None, ("partner", "block")),
            P(("partner", "block")),
            P(("partner", "block"), None, None, None),
            P(("partner", "block"), None),
            P(("partner", "block"), None, None),
            P(("partner", "block"), None, None),
            P(("partner", "block"), None, None),
            P(None, ("partner", "block"), None, None, None),
            P(),
        ),
        out_specs=P(None, ("partner", "block")),
        check_vma=False,
    )
```

```python
import functools

import jax
import jax.numpy as jnp
from jax import lax
from jax.experimental import pallas as pl
from jax.experimental.pallas import tpu as pltpu
from jax.sharding import PartitionSpec as P


REACH = 2
LANES = 128
VMEM = pl.BlockSpec(memory_space=pltpu.VMEM)
HBM = pl.BlockSpec(memory_space=pltpu.HBM)


def call(body, outs, in_specs, scratch=(), flops=1 << 20, moved=1 << 18, place=VMEM):
    single = not isinstance(outs, (list, tuple))
    run = pl.pallas_call(
        body,
        out_shape=outs,
        in_specs=in_specs,
        out_specs=place if single else [VMEM] * len(outs),
        scratch_shapes=list(scratch),
        compiler_params=pltpu.CompilerParams(vmem_limit_bytes=16 << 20),
        cost_estimate=pl.CostEstimate(flops=flops, bytes_accessed=moved, transcendentals=0),
    )

    def bound(*args):
        return run(
            *[
                pltpu.with_memory_space_constraint(a, pltpu.HBM) if s is HBM else a
                for a, s in zip(args, in_specs)
            ]
        )

    return bound


def tables(map_ref, row, slot_ref, rank_ref, slots):
    mask = jnp.int32(0)
    for i in range(slots):
        mask = mask | (jnp.int32(1) << map_ref[row, i])
    rank = jnp.int32(0)
    for j in range(slots):
        slot_ref[rank] = jnp.int32(j)
        rank_ref[j] = rank
        rank = rank + ((mask >> j) & 1)


class Places:
    def __init__(self, levels, leaves, near_count):
        self.leaves, self.half = leaves, leaves // 2
        self.level_rows = leaves + 2 * self.half
        self.near_base = levels * self.level_rows
        self.near_count = near_count
        self.rows = -(-(self.near_base + leaves * near_count) // 8) * 8

    def piece(self, level, i):
        return level * self.level_rows + i

    def slot(self, level, k):
        return level * self.level_rows + self.leaves + k

    def slot_piece(self, level, k):
        return level * self.level_rows + self.leaves + self.half + k

    def near(self, leaf, n):
        return self.near_base + leaf * self.near_count + n


def read(table, row):
    return table[pl.ds(row, 1), :][0, 0]


def split(x):
    high = x.astype(jnp.bfloat16)
    low = (x - high.astype(jnp.float32)).astype(jnp.bfloat16)
    return jnp.concatenate([high, low], axis=0)


def times(pair, factor):
    both = jnp.dot(pair, factor, preferred_element_type=jnp.float32)
    rows = both.shape[0] // 2
    return both[:rows] + both[rows:]


def pick_lanes(blocks, high, low):
    rows = blocks[0].shape[0]
    high = jnp.broadcast_to(high, (rows, LANES))
    low = jnp.broadcast_to(low, (rows, LANES))
    out = jnp.take_along_axis(blocks[0], low, axis=1)
    for b in range(1, len(blocks)):
        out = jnp.where(high == b, jnp.take_along_axis(blocks[b], low, axis=1), out)
    return out


def column_blocks(x, leaves):
    return [x[:, b * LANES : (b + 1) * LANES].astype(jnp.float32) for b in range(leaves)]


def first_body(
    places, points, order, compress, block_map, near,
    sent, table, pts, idx, comp, maps, nears, slots, ranks, sems,
):
    leaves = idx.shape[0]
    levels = maps.shape[0]
    copies = [
        pltpu.make_async_copy(block_map, maps, sems.at[0]),
        pltpu.make_async_copy(near, nears, sems.at[1]),
        pltpu.make_async_copy(order, idx, sems.at[2]),
        pltpu.make_async_copy(points, pts, sems.at[3]),
        pltpu.make_async_copy(compress, comp, sems.at[4]),
    ]
    for copy in copies:
        copy.start()

    def put(row, value):
        table[pl.ds(row, 1), :] = jnp.full((1, LANES), value, jnp.int32)

    copies[0].wait()
    for level in range(levels):
        slot, rank = slots.at[level], ranks.at[level]
        tables(maps, level, slot, rank, leaves)
        for i in range(leaves):
            put(places.piece(level, i), rank[maps[level, i]])
        if level > 0:
            for k in range(leaves // 2):
                i = slot[k]
                put(places.slot(level, k), i)
                put(places.slot_piece(level, k), ranks[level - 1, maps[level - 1, i]])
    copies[1].wait()
    device = lax.axis_index("partner") * lax.axis_size("block") + lax.axis_index("block")
    base = device * leaves
    for leaf in range(leaves):
        for n in range(nears.shape[0]):
            put(places.near(leaf, n), nears[n, leaf] - base + REACH)
    copies[2].wait()
    copies[3].wait()
    blocks = column_blocks(pts[...], leaves)
    rows = []
    for k in range(leaves // 2):
        local = idx[pl.ds(slots[0, k], 1), :] & (leaves * LANES - 1)
        rows.append(pick_lanes(blocks, local >> 7, local & (LANES - 1)).astype(jnp.bfloat16))
    copies[4].wait()
    for k in range(leaves // 2):
        product = jnp.dot(rows[k], comp[slots[0, k]], preferred_element_type=jnp.float32)
        sent[k] = split(product)


def order_body(points, order, ordered, even, odd):
    leaves = order.shape[0]
    blocks = column_blocks(points[...], leaves)
    for leaf in range(leaves):
        local = order[pl.ds(leaf, 1), :] & (leaves * LANES - 1)
        ordered[leaf] = pick_lanes(blocks, local >> 7, local & (LANES - 1)).astype(jnp.bfloat16)
    parity = lax.axis_index("block") & 1
    head, tail = 0, leaves - REACH
    even[...] = ordered[pl.ds(jnp.where(parity == 0, tail, head), REACH)]
    odd[...] = ordered[pl.ds(jnp.where(parity == 0, head, tail), REACH)]


def prep_body(
    order, expand, mixers_in, place, joint_own, joint, mixers, sem
):
    leaves = order.shape[0]
    copy = pltpu.make_async_copy(mixers_in, mixers, sem)
    copy.start()
    count = leaves * LANES
    target = lax.broadcasted_iota(jnp.int32, (count, LANES), 0)
    kind = lax.broadcasted_iota(jnp.int32, (8, LANES), 0)
    lane = lax.broadcasted_iota(jnp.int32, (8, LANES), 1)
    total = None
    for leaf in range(leaves):
        local = order[pl.ds(leaf, 1), :] & (count - 1)
        hit = jnp.where(target == local, 1.0, 0.0).astype(jnp.bfloat16)
        value = jnp.where(kind == 0, leaf, lane).astype(jnp.float32).astype(jnp.bfloat16)
        term = lax.dot_general(
            value, hit, (((1,), (1,)), ((), ())), preferred_element_type=jnp.float32
        )
        total = term if total is None else total + term
    place[...] = total.astype(jnp.int32)
    copy.wait()
    for side, out in enumerate((joint_own, joint)):
        for i in range(leaves):
            both = jnp.dot(
                mixers[mixers.shape[0] - 1, i, side], expand[i], preferred_element_type=jnp.float32
            )
            high = both.astype(jnp.bfloat16)
            out[i, :, :LANES] = high
            out[i, :, LANES:] = (both - high.astype(jnp.float32)).astype(jnp.bfloat16)


def top_send_body(places, table, received, factor, sent):
    for k in range(sent.shape[0]):
        i = read(table, places.slot(1, k))
        sent[k] = split(times(received[read(table, places.slot_piece(1, k))], factor[i]))


def top_own_body(places, table, received, factor, mixers, own):
    for i in range(own.shape[0]):
        state = split(times(received[read(table, places.piece(0, i))], factor[i]))
        own[i] = times(state, mixers[0, i, 0])


def mix_send_body(places, level, table, received, own, mixers, sent):
    for k in range(sent.shape[0]):
        i = read(table, places.slot(level + 1, k))
        piece = received[read(table, places.slot_piece(level + 1, k))]
        sent[k] = split(own[i] + times(piece, mixers[level - 1, i, 1]))


def mix_own_body(places, level, table, received, own, mixers, own_next):
    for i in range(own.shape[0]):
        other = times(received[read(table, places.piece(level, i))], mixers[level - 1, i, 1])
        own_next[i] = times(split(own[i] + other), mixers[level, i, 0])


def times_joint(pair, joint):
    both = jnp.dot(pair, joint, preferred_element_type=jnp.float32)
    rows = both.shape[0] // 2
    return (both[:rows, :LANES] + both[rows:, :LANES]) + (both[:rows, LANES:] + both[rows:, LANES:])


def base_body(
    places, level, table, received, own, mixers, joint_own, even, ordered, odd, dense, base, windows
):
    leaves, near_count = dense.shape[0], dense.shape[1]
    parity = lax.axis_index("block") & 1
    first, last = 0, leaves + REACH
    windows[pl.ds(jnp.where(parity == 0, last, first), REACH)] = even[...]
    windows[pl.ds(jnp.where(parity == 0, first, last), REACH)] = odd[...]
    windows[pl.ds(REACH, leaves)] = ordered[...]
    for i in range(leaves):
        other = times(received[read(table, places.piece(level, i))], mixers[level - 1, i, 1])
        total = times_joint(split(own[i] + other), joint_own[i])
        for n in range(near_count):
            source = windows[read(table, places.near(i, n))]
            total = total + jnp.dot(source, dense[i, n], preferred_element_type=jnp.float32)
        base[i] = total


def last_body(places, level, table, received, base, joint, place, applied, rows, sems):
    leaves = base.shape[0]
    blocks = []
    for i in range(leaves):
        piece = received[read(table, places.piece(level, i))]
        blocks.append((base[i] + times_joint(piece, joint[i])).astype(jnp.bfloat16).astype(jnp.float32))
    group = rows.shape[0] // sems.shape[0]
    copies = []
    for g in range(sems.shape[0]):
        here = slice(g * group, (g + 1) * group)
        part = [block[here] for block in blocks]
        for b in range(leaves):
            lanes = slice(b * LANES, (b + 1) * LANES)
            picked = pick_lanes(part, place[pl.ds(0, 1), lanes], place[pl.ds(1, 1), lanes])
            rows[here, lanes] = picked.astype(jnp.bfloat16)
        copies.append(pltpu.make_async_copy(rows.at[here], applied.at[here], sems.at[g]))
        copies[-1].start()
    for copy in copies:
        copy.wait()


def from_partner(x, bit):
    count = lax.axis_size("partner")
    return lax.ppermute(x, "partner", [(i, i ^ 1 << bit) for i in range(count)])


def with_neighbour(x, first):
    groups, count = lax.axis_size("partner"), lax.axis_size("block")
    to = {}
    for g in range(groups):
        for i in range(count):
            to[g * count + i] = (g ^ 1) * count + i
        for i in range(first, count - 1, 2):
            to[g * count + i], to[g * count + i + 1] = g * count + i + 1, g * count + i
    return lax.ppermute(x, ("partner", "block"), sorted(to.items()))


def on_device(
    points,
    tree_order,
    nearby_dense_blocks,
    neighbours,
    compress,
    expand,
    top_factor,
    butterfly_mixers,
    block_map,
):
    vectors, count = points.shape
    leaves, near_count = neighbours.shape
    levels = lax.axis_size("partner").bit_length() - 1
    half = leaves // 2
    places = Places(levels, leaves, near_count)
    order = tree_order.reshape(leaves, LANES)
    ints = pltpu.SMEM((levels, leaves + 1), jnp.int32)
    pair = jax.ShapeDtypeStruct((half, 2 * vectors, LANES), jnp.bfloat16)
    state = jax.ShapeDtypeStruct((leaves, vectors, LANES), jnp.float32)
    edge = jax.ShapeDtypeStruct((REACH, vectors, LANES), jnp.bfloat16)
    part = functools.partial
    assert levels > 2

    sent, table = call(
        part(first_body, places),
        [pair, jax.ShapeDtypeStruct((places.rows, LANES), jnp.int32)],
        [HBM] * 5,
        [
            pltpu.VMEM(points.shape, points.dtype),
            pltpu.VMEM(order.shape, order.dtype),
            pltpu.VMEM(compress.shape, compress.dtype),
            pltpu.SMEM(block_map.shape, block_map.dtype),
            pltpu.SMEM((near_count, leaves), neighbours.dtype),
            ints,
            ints,
            pltpu.SemaphoreType.DMA((5,)),
        ],
    )(points, order, compress, block_map, neighbours.T)
    received = from_partner(sent, levels - 1)

    ordered, even, odd = call(
        order_body,
        [jax.ShapeDtypeStruct((leaves, vectors, LANES), jnp.bfloat16), edge, edge],
        [VMEM] * 2,
        flops=1 << 24,
    )(points, order)
    even = with_neighbour(even, 0)
    odd = with_neighbour(odd, 1)

    sent = call(part(top_send_body, places), pair, [VMEM] * 3)(table, received, top_factor)
    wide = jax.ShapeDtypeStruct((leaves, LANES, 2 * LANES), jnp.bfloat16)
    place, joint_own, joint, mixers = call(
        prep_body,
        [
            jax.ShapeDtypeStruct((8, count), jnp.int32),
            wide,
            wide,
            jax.ShapeDtypeStruct(butterfly_mixers.shape, butterfly_mixers.dtype),
        ],
        [VMEM, VMEM, HBM],
        [pltpu.SemaphoreType.DMA],
        flops=1 << 24,
    )(order, expand, butterfly_mixers)
    own = call(part(top_own_body, places), state, [VMEM] * 4, flops=1 << 24)(
        table, received, top_factor, mixers
    )

    for level in range(1, levels):
        received = from_partner(sent, levels - 1 - level)
        if level < levels - 1:
            sent = call(part(mix_send_body, places, level), pair, [VMEM] * 4)(
                table, received, own, mixers
            )
            if level < levels - 2:
                body, factors, scratch = mix_own_body, (mixers,), ()
            else:
                body = base_body
                factors = (mixers, joint_own, even, ordered, odd, nearby_dense_blocks)
                scratch = [pltpu.VMEM((leaves + 2 * REACH, vectors, LANES), jnp.bfloat16)]
            own = call(
                part(body, places, level),
                state,
                [VMEM] * (3 + len(factors)),
                scratch,
                flops=1 << 24,
            )(table, received, own, *factors)
    return call(
        part(last_body, places, levels - 1),
        jax.ShapeDtypeStruct(points.shape, points.dtype),
        [VMEM] * 5,
        [pltpu.VMEM(points.shape, points.dtype), pltpu.SemaphoreType.DMA((2,))],
        place=HBM,
    )(table, received, own, joint, place)


def solution(mesh):
    return jax.shard_map(
        on_device,
        mesh=mesh,
        in_specs=(
            P(None, ("partner", "block")),
            P(("partner", "block")),
            P(("partner", "block"), None, None, None),
            P(("partner", "block"), None),
            P(("partner", "block"), None, None),
            P(("partner", "block"), None, None),
            P(("partner", "block"), None, None),
            P(None, ("partner", "block"), None, None, None),
            P(),
        ),
        out_specs=P(None, ("partner", "block")),
        check_vma=False,
    )
```

```python
import functools

import jax
import jax.numpy as jnp
from jax import lax
from jax.experimental import pallas as pl
from jax.experimental.pallas import tpu as pltpu
from jax.sharding import PartitionSpec as P


REACH = 2
LANES = 128
VMEM = pl.BlockSpec(memory_space=pltpu.VMEM)
HBM = pl.BlockSpec(memory_space=pltpu.HBM)


def call(body, outs, in_specs, scratch=(), flops=1 << 20, moved=1 << 18, place=VMEM):
    single = not isinstance(outs, (list, tuple))
    run = pl.pallas_call(
        body,
        out_shape=outs,
        in_specs=in_specs,
        out_specs=place if single else [VMEM] * len(outs),
        scratch_shapes=list(scratch),
        compiler_params=pltpu.CompilerParams(vmem_limit_bytes=16 << 20),
        cost_estimate=pl.CostEstimate(flops=flops, bytes_accessed=moved, transcendentals=0),
    )

    def bound(*args):
        return run(
            *[
                pltpu.with_memory_space_constraint(a, pltpu.HBM) if s is HBM else a
                for a, s in zip(args, in_specs)
            ]
        )

    return bound


def tables(map_ref, row, slot_ref, rank_ref, slots):
    mask = jnp.int32(0)
    for i in range(slots):
        mask = mask | (jnp.int32(1) << map_ref[row, i])
    rank = jnp.int32(0)
    for j in range(slots):
        slot_ref[rank] = jnp.int32(j)
        rank_ref[j] = rank
        rank = rank + ((mask >> j) & 1)


class Places:
    def __init__(self, levels, leaves, near_count):
        self.leaves, self.half = leaves, leaves // 2
        self.level_rows = leaves + 2 * self.half
        self.near_base = levels * self.level_rows
        self.near_count = near_count
        self.rows = -(-(self.near_base + leaves * near_count) // 8) * 8

    def piece(self, level, i):
        return level * self.level_rows + i

    def slot(self, level, k):
        return level * self.level_rows + self.leaves + k

    def slot_piece(self, level, k):
        return level * self.level_rows + self.leaves + self.half + k

    def near(self, leaf, n):
        return self.near_base + leaf * self.near_count + n


def read(table, row):
    return table[pl.ds(row, 1), :][0, 0]


def split(x):
    high = x.astype(jnp.bfloat16)
    low = (x - high.astype(jnp.float32)).astype(jnp.bfloat16)
    return jnp.concatenate([high, low], axis=0)


def times(pair, factor):
    both = jnp.dot(pair, factor, preferred_element_type=jnp.float32)
    rows = both.shape[0] // 2
    return both[:rows] + both[rows:]


def pick_lanes(blocks, high, low):
    rows = blocks[0].shape[0]
    high = jnp.broadcast_to(high, (rows, LANES))
    low = jnp.broadcast_to(low, (rows, LANES))
    out = jnp.take_along_axis(blocks[0], low, axis=1)
    for b in range(1, len(blocks)):
        out = jnp.where(high == b, jnp.take_along_axis(blocks[b], low, axis=1), out)
    return out


def column_blocks(x, leaves):
    return [x[:, b * LANES : (b + 1) * LANES].astype(jnp.float32) for b in range(leaves)]


def first_body(
    places, points, order, compress, block_map, near,
    sent, table, pts, idx, comp, maps, nears, slots, ranks, sems,
):
    leaves = idx.shape[0]
    levels = maps.shape[0]
    copies = [
        pltpu.make_async_copy(block_map, maps, sems.at[0]),
        pltpu.make_async_copy(near, nears, sems.at[1]),
        pltpu.make_async_copy(order, idx, sems.at[2]),
        pltpu.make_async_copy(points, pts, sems.at[3]),
        pltpu.make_async_copy(compress, comp, sems.at[4]),
    ]
    for copy in copies:
        copy.start()

    def put(row, value):
        table[pl.ds(row, 1), :] = jnp.full((1, LANES), value, jnp.int32)

    copies[0].wait()
    for level in range(levels):
        slot, rank = slots.at[level], ranks.at[level]
        tables(maps, level, slot, rank, leaves)
        for i in range(leaves):
            put(places.piece(level, i), rank[maps[level, i]])
        if level > 0:
            for k in range(leaves // 2):
                i = slot[k]
                put(places.slot(level, k), i)
                put(places.slot_piece(level, k), ranks[level - 1, maps[level - 1, i]])
    copies[1].wait()
    device = lax.axis_index("partner") * lax.axis_size("block") + lax.axis_index("block")
    base = device * leaves
    for leaf in range(leaves):
        for n in range(nears.shape[0]):
            put(places.near(leaf, n), nears[n, leaf] - base + REACH)
    copies[2].wait()
    copies[3].wait()
    blocks = column_blocks(pts[...], leaves)
    rows = []
    for k in range(leaves // 2):
        local = idx[pl.ds(slots[0, k], 1), :] & (leaves * LANES - 1)
        rows.append(pick_lanes(blocks, local >> 7, local & (LANES - 1)).astype(jnp.bfloat16))
    copies[4].wait()
    for k in range(leaves // 2):
        product = jnp.dot(rows[k], comp[slots[0, k]], preferred_element_type=jnp.float32)
        sent[k] = split(product)


def order_body(points, order, ordered, even, odd):
    leaves = order.shape[0]
    blocks = column_blocks(points[...], leaves)
    for leaf in range(leaves):
        local = order[pl.ds(leaf, 1), :] & (leaves * LANES - 1)
        ordered[leaf] = pick_lanes(blocks, local >> 7, local & (LANES - 1)).astype(jnp.bfloat16)
    parity = lax.axis_index("block") & 1
    head, tail = 0, leaves - REACH
    even[...] = ordered[pl.ds(jnp.where(parity == 0, tail, head), REACH)]
    odd[...] = ordered[pl.ds(jnp.where(parity == 0, head, tail), REACH)]


def prep_body(
    order, expand, mixers_in, place, joint_own, joint, mixers, sem
):
    leaves = order.shape[0]
    copy = pltpu.make_async_copy(mixers_in, mixers, sem)
    copy.start()
    count = leaves * LANES
    target = lax.broadcasted_iota(jnp.int32, (count, LANES), 0)
    kind = lax.broadcasted_iota(jnp.int32, (8, LANES), 0)
    lane = lax.broadcasted_iota(jnp.int32, (8, LANES), 1)
    total = None
    for leaf in range(leaves):
        local = order[pl.ds(leaf, 1), :] & (count - 1)
        hit = jnp.where(target == local, 1.0, 0.0).astype(jnp.bfloat16)
        value = jnp.where(kind == 0, leaf, lane).astype(jnp.float32).astype(jnp.bfloat16)
        term = lax.dot_general(
            value, hit, (((1,), (1,)), ((), ())), preferred_element_type=jnp.float32
        )
        total = term if total is None else total + term
    place[...] = total.astype(jnp.int32)
    copy.wait()
    for side, out in enumerate((joint_own, joint)):
        for i in range(leaves):
            both = jnp.dot(
                mixers[mixers.shape[0] - 1, i, side], expand[i], preferred_element_type=jnp.float32
            )
            high = both.astype(jnp.bfloat16)
            out[i, :, :LANES] = high
            out[i, :, LANES:] = (both - high.astype(jnp.float32)).astype(jnp.bfloat16)


def top_send_body(places, table, received, factor, sent):
    for k in range(sent.shape[0]):
        i = read(table, places.slot(1, k))
        sent[k] = split(times(received[read(table, places.slot_piece(1, k))], factor[i]))


def top_own_body(places, table, received, factor, mixers, dense, own):
    for i in range(own.shape[0]):
        state = split(times(received[read(table, places.piece(0, i))], factor[i]))
        own[i] = times(state, mixers[0, i, 0])


def mix_send_body(places, level, table, received, own, mixers, sent):
    for k in range(sent.shape[0]):
        i = read(table, places.slot(level + 1, k))
        piece = received[read(table, places.slot_piece(level + 1, k))]
        sent[k] = split(own[i] + times(piece, mixers[level - 1, i, 1]))


def mix_own_body(places, level, table, received, own, mixers, own_next):
    for i in range(own.shape[0]):
        other = times(received[read(table, places.piece(level, i))], mixers[level - 1, i, 1])
        own_next[i] = times(split(own[i] + other), mixers[level, i, 0])


def times_joint(pair, joint):
    both = jnp.dot(pair, joint, preferred_element_type=jnp.float32)
    rows = both.shape[0] // 2
    return (both[:rows, :LANES] + both[rows:, :LANES]) + (both[:rows, LANES:] + both[rows:, LANES:])


def base_body(
    places, level, table, received, own, mixers, joint_own, even, ordered, odd, dense, base, windows
):
    leaves, near_count = dense.shape[0], dense.shape[1]
    parity = lax.axis_index("block") & 1
    first, last = 0, leaves + REACH
    windows[pl.ds(jnp.where(parity == 0, last, first), REACH)] = even[...]
    windows[pl.ds(jnp.where(parity == 0, first, last), REACH)] = odd[...]
    windows[pl.ds(REACH, leaves)] = ordered[...]
    for i in range(leaves):
        other = times(received[read(table, places.piece(level, i))], mixers[level - 1, i, 1])
        total = times_joint(split(own[i] + other), joint_own[i])
        for n in range(near_count):
            source = windows[read(table, places.near(i, n))]
            total = total + jnp.dot(source, dense[i, n], preferred_element_type=jnp.float32)
        base[i] = total


def last_body(places, level, table, received, base, joint, place, applied, rows, sems):
    leaves = base.shape[0]
    blocks = []
    for i in range(leaves):
        piece = received[read(table, places.piece(level, i))]
        blocks.append((base[i] + times_joint(piece, joint[i])).astype(jnp.bfloat16).astype(jnp.float32))
    group = rows.shape[0] // sems.shape[0]
    copies = []
    for g in range(sems.shape[0]):
        here = slice(g * group, (g + 1) * group)
        part = [block[here] for block in blocks]
        for b in range(leaves):
            lanes = slice(b * LANES, (b + 1) * LANES)
            picked = pick_lanes(part, place[pl.ds(0, 1), lanes], place[pl.ds(1, 1), lanes])
            rows[here, lanes] = picked.astype(jnp.bfloat16)
        copies.append(pltpu.make_async_copy(rows.at[here], applied.at[here], sems.at[g]))
        copies[-1].start()
    for copy in copies:
        copy.wait()


def from_partner(x, bit):
    count = lax.axis_size("partner")
    return lax.ppermute(x, "partner", [(i, i ^ 1 << bit) for i in range(count)])


def with_neighbour(x, first):
    groups, count = lax.axis_size("partner"), lax.axis_size("block")
    to = {}
    for g in range(groups):
        for i in range(count):
            to[g * count + i] = (g ^ 1) * count + i
        for i in range(first, count - 1, 2):
            to[g * count + i], to[g * count + i + 1] = g * count + i + 1, g * count + i
    return lax.ppermute(x, ("partner", "block"), sorted(to.items()))


def on_device(
    points,
    tree_order,
    nearby_dense_blocks,
    neighbours,
    compress,
    expand,
    top_factor,
    butterfly_mixers,
    block_map,
):
    vectors, count = points.shape
    leaves, near_count = neighbours.shape
    levels = lax.axis_size("partner").bit_length() - 1
    half = leaves // 2
    places = Places(levels, leaves, near_count)
    order = tree_order.reshape(leaves, LANES)
    ints = pltpu.SMEM((levels, leaves + 1), jnp.int32)
    pair = jax.ShapeDtypeStruct((half, 2 * vectors, LANES), jnp.bfloat16)
    state = jax.ShapeDtypeStruct((leaves, vectors, LANES), jnp.float32)
    edge = jax.ShapeDtypeStruct((REACH, vectors, LANES), jnp.bfloat16)
    part = functools.partial
    assert levels > 2

    sent, table = call(
        part(first_body, places),
        [pair, jax.ShapeDtypeStruct((places.rows, LANES), jnp.int32)],
        [HBM] * 5,
        [
            pltpu.VMEM(points.shape, points.dtype),
            pltpu.VMEM(order.shape, order.dtype),
            pltpu.VMEM(compress.shape, compress.dtype),
            pltpu.SMEM(block_map.shape, block_map.dtype),
            pltpu.SMEM((near_count, leaves), neighbours.dtype),
            ints,
            ints,
            pltpu.SemaphoreType.DMA((5,)),
        ],
    )(points, order, compress, block_map, neighbours.T)
    received = from_partner(sent, levels - 1)

    ordered, even, odd = call(
        order_body,
        [jax.ShapeDtypeStruct((leaves, vectors, LANES), jnp.bfloat16), edge, edge],
        [VMEM] * 2,
        flops=1 << 24,
    )(points, order)
    even = with_neighbour(even, 0)
    odd = with_neighbour(odd, 1)

    sent = call(part(top_send_body, places), pair, [VMEM] * 3)(table, received, top_factor)
    wide = jax.ShapeDtypeStruct((leaves, LANES, 2 * LANES), jnp.bfloat16)
    place, joint_own, joint, mixers = call(
        prep_body,
        [
            jax.ShapeDtypeStruct((8, count), jnp.int32),
            wide,
            wide,
            jax.ShapeDtypeStruct(butterfly_mixers.shape, butterfly_mixers.dtype),
        ],
        [VMEM, VMEM, HBM],
        [pltpu.SemaphoreType.DMA],
        flops=1 << 24,
    )(order, expand, butterfly_mixers)
    own = call(part(top_own_body, places), state, [VMEM] * 5, flops=1 << 24)(
        table, received, top_factor, mixers, nearby_dense_blocks
    )

    for level in range(1, levels):
        received = from_partner(sent, levels - 1 - level)
        if level < levels - 1:
            sent = call(part(mix_send_body, places, level), pair, [VMEM] * 4)(
                table, received, own, mixers
            )
            if level < levels - 2:
                body, factors, scratch = mix_own_body, (mixers,), ()
            else:
                body = base_body
                factors = (mixers, joint_own, even, ordered, odd, nearby_dense_blocks)
                scratch = [pltpu.VMEM((leaves + 2 * REACH, vectors, LANES), jnp.bfloat16)]
            own = call(
                part(body, places, level),
                state,
                [VMEM] * (3 + len(factors)),
                scratch,
                flops=1 << 24,
            )(table, received, own, *factors)
    return call(
        part(last_body, places, levels - 1),
        jax.ShapeDtypeStruct(points.shape, points.dtype),
        [VMEM] * 5,
        [pltpu.VMEM(points.shape, points.dtype), pltpu.SemaphoreType.DMA((2,))],
        place=HBM,
    )(table, received, own, joint, place)


def solution(mesh):
    return jax.shard_map(
        on_device,
        mesh=mesh,
        in_specs=(
            P(None, ("partner", "block")),
            P(("partner", "block")),
            P(("partner", "block"), None, None, None),
            P(("partner", "block"), None),
            P(("partner", "block"), None, None),
            P(("partner", "block"), None, None),
            P(("partner", "block"), None, None),
            P(None, ("partner", "block"), None, None, None),
            P(),
        ),
        out_specs=P(None, ("partner", "block")),
        check_vma=False,
    )
```

```python
import functools

import jax
import jax.numpy as jnp
from jax import lax
from jax.experimental import pallas as pl
from jax.experimental.pallas import tpu as pltpu
from jax.sharding import PartitionSpec as P


REACH = 2
LANES = 128
VMEM = pl.BlockSpec(memory_space=pltpu.VMEM)
HBM = pl.BlockSpec(memory_space=pltpu.HBM)


def call(body, outs, in_specs, scratch=(), flops=1 << 20, moved=1 << 18, place=VMEM):
    single = not isinstance(outs, (list, tuple))
    run = pl.pallas_call(
        body,
        out_shape=outs,
        in_specs=in_specs,
        out_specs=place if single else [VMEM] * len(outs),
        scratch_shapes=list(scratch),
        compiler_params=pltpu.CompilerParams(vmem_limit_bytes=16 << 20),
        cost_estimate=pl.CostEstimate(flops=flops, bytes_accessed=moved, transcendentals=0),
    )

    def bound(*args):
        return run(
            *[
                pltpu.with_memory_space_constraint(a, pltpu.HBM) if s is HBM else a
                for a, s in zip(args, in_specs)
            ]
        )

    return bound


def tables(map_ref, row, slot_ref, rank_ref, slots):
    mask = jnp.int32(0)
    for i in range(slots):
        mask = mask | (jnp.int32(1) << map_ref[row, i])
    rank = jnp.int32(0)
    for j in range(slots):
        slot_ref[rank] = jnp.int32(j)
        rank_ref[j] = rank
        rank = rank + ((mask >> j) & 1)


class Places:
    def __init__(self, levels, leaves, near_count):
        self.leaves, self.half = leaves, leaves // 2
        self.level_rows = leaves + 2 * self.half
        self.near_base = levels * self.level_rows
        self.near_count = near_count
        self.rows = -(-(self.near_base + leaves * near_count) // 8) * 8

    def piece(self, level, i):
        return level * self.level_rows + i

    def slot(self, level, k):
        return level * self.level_rows + self.leaves + k

    def slot_piece(self, level, k):
        return level * self.level_rows + self.leaves + self.half + k

    def near(self, leaf, n):
        return self.near_base + leaf * self.near_count + n


def read(table, row):
    return table[pl.ds(row, 1), :][0, 0]


def split(x):
    high = x.astype(jnp.bfloat16)
    low = (x - high.astype(jnp.float32)).astype(jnp.bfloat16)
    return jnp.concatenate([high, low], axis=0)


def times(pair, factor):
    both = jnp.dot(pair, factor, preferred_element_type=jnp.float32)
    rows = both.shape[0] // 2
    return both[:rows] + both[rows:]


def pick_lanes(blocks, high, low):
    rows = blocks[0].shape[0]
    high = jnp.broadcast_to(high, (rows, LANES))
    low = jnp.broadcast_to(low, (rows, LANES))
    out = jnp.take_along_axis(blocks[0], low, axis=1)
    for b in range(1, len(blocks)):
        out = jnp.where(high == b, jnp.take_along_axis(blocks[b], low, axis=1), out)
    return out


def column_blocks(x, leaves):
    return [x[:, b * LANES : (b + 1) * LANES].astype(jnp.float32) for b in range(leaves)]


def first_body(
    places, points, order, compress, block_map, near,
    sent, table, pts, idx, comp, maps, nears, slots, ranks, sems,
):
    leaves = idx.shape[0]
    levels = maps.shape[0]
    copies = [
        pltpu.make_async_copy(block_map, maps, sems.at[0]),
        pltpu.make_async_copy(near, nears, sems.at[1]),
        pltpu.make_async_copy(order, idx, sems.at[2]),
        pltpu.make_async_copy(points, pts, sems.at[3]),
        pltpu.make_async_copy(compress, comp, sems.at[4]),
    ]
    for copy in copies:
        copy.start()

    def put(row, value):
        table[pl.ds(row, 1), :] = jnp.full((1, LANES), value, jnp.int32)

    copies[0].wait()
    for level in range(levels):
        slot, rank = slots.at[level], ranks.at[level]
        tables(maps, level, slot, rank, leaves)
        for i in range(leaves):
            put(places.piece(level, i), rank[maps[level, i]])
        if level > 0:
            for k in range(leaves // 2):
                i = slot[k]
                put(places.slot(level, k), i)
                put(places.slot_piece(level, k), ranks[level - 1, maps[level - 1, i]])
    copies[1].wait()
    device = lax.axis_index("partner") * lax.axis_size("block") + lax.axis_index("block")
    base = device * leaves
    for leaf in range(leaves):
        for n in range(nears.shape[0]):
            put(places.near(leaf, n), nears[n, leaf] - base + REACH)
    copies[2].wait()
    copies[3].wait()
    blocks = column_blocks(pts[...], leaves)
    rows = []
    for k in range(leaves // 2):
        local = idx[pl.ds(slots[0, k], 1), :] & (leaves * LANES - 1)
        rows.append(pick_lanes(blocks, local >> 7, local & (LANES - 1)).astype(jnp.bfloat16))
    copies[4].wait()
    for k in range(leaves // 2):
        product = jnp.dot(rows[k], comp[slots[0, k]], preferred_element_type=jnp.float32)
        sent[k] = split(product)


def order_body(points, order, ordered, even, odd):
    leaves = order.shape[0]
    blocks = column_blocks(points[...], leaves)
    for leaf in range(leaves):
        local = order[pl.ds(leaf, 1), :] & (leaves * LANES - 1)
        ordered[leaf] = pick_lanes(blocks, local >> 7, local & (LANES - 1)).astype(jnp.bfloat16)
    parity = lax.axis_index("block") & 1
    head, tail = 0, leaves - REACH
    even[...] = ordered[pl.ds(jnp.where(parity == 0, tail, head), REACH)]
    odd[...] = ordered[pl.ds(jnp.where(parity == 0, head, tail), REACH)]


def prep_body(
    places, table, received, factor, order, expand, mixers_in,
    own, place, joint_own, joint, mixers, sem,
):
    leaves = order.shape[0]
    copy = pltpu.make_async_copy(mixers_in, mixers, sem)
    copy.start()
    count = leaves * LANES
    target = lax.broadcasted_iota(jnp.int32, (count, LANES), 0)
    kind = lax.broadcasted_iota(jnp.int32, (8, LANES), 0)
    lane = lax.broadcasted_iota(jnp.int32, (8, LANES), 1)
    total = None
    for leaf in range(leaves):
        local = order[pl.ds(leaf, 1), :] & (count - 1)
        hit = jnp.where(target == local, 1.0, 0.0).astype(jnp.bfloat16)
        value = jnp.where(kind == 0, leaf, lane).astype(jnp.float32).astype(jnp.bfloat16)
        term = lax.dot_general(
            value, hit, (((1,), (1,)), ((), ())), preferred_element_type=jnp.float32
        )
        total = term if total is None else total + term
    place[...] = total.astype(jnp.int32)
    states = []
    for i in range(leaves):
        states.append(split(times(received[read(table, places.piece(0, i))], factor[i])))
    copy.wait()
    for i in range(leaves):
        own[i] = times(states[i], mixers[0, i, 0])
    for side, out in enumerate((joint_own, joint)):
        for i in range(leaves):
            both = jnp.dot(
                mixers[mixers.shape[0] - 1, i, side], expand[i], preferred_element_type=jnp.float32
            )
            high = both.astype(jnp.bfloat16)
            out[i, :, :LANES] = high
            out[i, :, LANES:] = (both - high.astype(jnp.float32)).astype(jnp.bfloat16)


def top_send_body(places, table, received, factor, sent):
    for k in range(sent.shape[0]):
        i = read(table, places.slot(1, k))
        sent[k] = split(times(received[read(table, places.slot_piece(1, k))], factor[i]))


def mix_send_body(places, level, table, received, own, mixers, dense, sent):
    for k in range(sent.shape[0]):
        i = read(table, places.slot(level + 1, k))
        piece = received[read(table, places.slot_piece(level + 1, k))]
        sent[k] = split(own[i] + times(piece, mixers[level - 1, i, 1]))


def mix_own_body(places, level, table, received, own, mixers, own_next):
    for i in range(own.shape[0]):
        other = times(received[read(table, places.piece(level, i))], mixers[level - 1, i, 1])
        own_next[i] = times(split(own[i] + other), mixers[level, i, 0])


def times_joint(pair, joint):
    both = jnp.dot(pair, joint, preferred_element_type=jnp.float32)
    rows = both.shape[0] // 2
    return (both[:rows, :LANES] + both[rows:, :LANES]) + (both[:rows, LANES:] + both[rows:, LANES:])


def base_body(
    places, level, table, received, own, mixers, joint_own, even, ordered, odd, dense, base, windows
):
    leaves, near_count = dense.shape[0], dense.shape[1]
    parity = lax.axis_index("block") & 1
    first, last = 0, leaves + REACH
    windows[pl.ds(jnp.where(parity == 0, last, first), REACH)] = even[...]
    windows[pl.ds(jnp.where(parity == 0, first, last), REACH)] = odd[...]
    windows[pl.ds(REACH, leaves)] = ordered[...]
    for i in range(leaves):
        other = times(received[read(table, places.piece(level, i))], mixers[level - 1, i, 1])
        total = times_joint(split(own[i] + other), joint_own[i])
        for n in range(near_count):
            source = windows[read(table, places.near(i, n))]
            total = total + jnp.dot(source, dense[i, n], preferred_element_type=jnp.float32)
        base[i] = total


def last_body(places, level, table, received, base, joint, place, applied, rows, sems):
    leaves = base.shape[0]
    blocks = []
    for i in range(leaves):
        piece = received[read(table, places.piece(level, i))]
        blocks.append((base[i] + times_joint(piece, joint[i])).astype(jnp.bfloat16).astype(jnp.float32))
    group = rows.shape[0] // sems.shape[0]
    copies = []
    for g in range(sems.shape[0]):
        here = slice(g * group, (g + 1) * group)
        part = [block[here] for block in blocks]
        for b in range(leaves):
            lanes = slice(b * LANES, (b + 1) * LANES)
            picked = pick_lanes(part, place[pl.ds(0, 1), lanes], place[pl.ds(1, 1), lanes])
            rows[here, lanes] = picked.astype(jnp.bfloat16)
        copies.append(pltpu.make_async_copy(rows.at[here], applied.at[here], sems.at[g]))
        copies[-1].start()
    for copy in copies:
        copy.wait()


def from_partner(x, bit):
    count = lax.axis_size("partner")
    return lax.ppermute(x, "partner", [(i, i ^ 1 << bit) for i in range(count)])


def with_neighbour(x, first):
    groups, count = lax.axis_size("partner"), lax.axis_size("block")
    to = {}
    for g in range(groups):
        for i in range(count):
            to[g * count + i] = (g ^ 1) * count + i
        for i in range(first, count - 1, 2):
            to[g * count + i], to[g * count + i + 1] = g * count + i + 1, g * count + i
    return lax.ppermute(x, ("partner", "block"), sorted(to.items()))


def on_device(
    points,
    tree_order,
    nearby_dense_blocks,
    neighbours,
    compress,
    expand,
    top_factor,
    butterfly_mixers,
    block_map,
):
    vectors, count = points.shape
    leaves, near_count = neighbours.shape
    levels = lax.axis_size("partner").bit_length() - 1
    half = leaves // 2
    places = Places(levels, leaves, near_count)
    order = tree_order.reshape(leaves, LANES)
    ints = pltpu.SMEM((levels, leaves + 1), jnp.int32)
    pair = jax.ShapeDtypeStruct((half, 2 * vectors, LANES), jnp.bfloat16)
    state = jax.ShapeDtypeStruct((leaves, vectors, LANES), jnp.float32)
    edge = jax.ShapeDtypeStruct((REACH, vectors, LANES), jnp.bfloat16)
    part = functools.partial
    assert levels > 2

    sent, table = call(
        part(first_body, places),
        [pair, jax.ShapeDtypeStruct((places.rows, LANES), jnp.int32)],
        [HBM] * 5,
        [
            pltpu.VMEM(points.shape, points.dtype),
            pltpu.VMEM(order.shape, order.dtype),
            pltpu.VMEM(compress.shape, compress.dtype),
            pltpu.SMEM(block_map.shape, block_map.dtype),
            pltpu.SMEM((near_count, leaves), neighbours.dtype),
            ints,
            ints,
            pltpu.SemaphoreType.DMA((5,)),
        ],
    )(points, order, compress, block_map, neighbours.T)
    received = from_partner(sent, levels - 1)

    ordered, even, odd = call(
        order_body,
        [jax.ShapeDtypeStruct((leaves, vectors, LANES), jnp.bfloat16), edge, edge],
        [VMEM] * 2,
        flops=1 << 24,
    )(points, order)
    even = with_neighbour(even, 0)
    odd = with_neighbour(odd, 1)

    sent = call(part(top_send_body, places), pair, [VMEM] * 3)(table, received, top_factor)
    wide = jax.ShapeDtypeStruct((leaves, LANES, 2 * LANES), jnp.bfloat16)
    own, place, joint_own, joint, mixers = call(
        part(prep_body, places),
        [
            state,
            jax.ShapeDtypeStruct((8, count), jnp.int32),
            wide,
            wide,
            jax.ShapeDtypeStruct(butterfly_mixers.shape, butterfly_mixers.dtype),
        ],
        [VMEM] * 5 + [HBM],
        [pltpu.SemaphoreType.DMA],
        flops=1 << 24,
    )(table, received, top_factor, order, expand, butterfly_mixers)

    for level in range(1, levels):
        received = from_partner(sent, levels - 1 - level)
        if level < levels - 1:
            sent = call(part(mix_send_body, places, level), pair, [VMEM] * 5)(
                table, received, own, mixers, nearby_dense_blocks
            )
            if level < levels - 2:
                body, factors, scratch = mix_own_body, (mixers,), ()
            else:
                body = base_body
                factors = (mixers, joint_own, even, ordered, odd, nearby_dense_blocks)
                scratch = [pltpu.VMEM((leaves + 2 * REACH, vectors, LANES), jnp.bfloat16)]
            own = call(
                part(body, places, level),
                state,
                [VMEM] * (3 + len(factors)),
                scratch,
                flops=1 << 24,
            )(table, received, own, *factors)
    return call(
        part(last_body, places, levels - 1),
        jax.ShapeDtypeStruct(points.shape, points.dtype),
        [VMEM] * 5,
        [pltpu.VMEM(points.shape, points.dtype), pltpu.SemaphoreType.DMA((2,))],
        place=HBM,
    )(table, received, own, joint, place)


def solution(mesh):
    return jax.shard_map(
        on_device,
        mesh=mesh,
        in_specs=(
            P(None, ("partner", "block")),
            P(("partner", "block")),
            P(("partner", "block"), None, None, None),
            P(("partner", "block"), None),
            P(("partner", "block"), None, None),
            P(("partner", "block"), None, None),
            P(("partner", "block"), None, None),
            P(None, ("partner", "block"), None, None, None),
            P(),
        ),
        out_specs=P(None, ("partner", "block")),
        check_vma=False,
    )
```

```python
import functools

import jax
import jax.numpy as jnp
from jax import lax
from jax.experimental import pallas as pl
from jax.experimental.pallas import tpu as pltpu
from jax.sharding import PartitionSpec as P


REACH = 2
LANES = 128
VMEM = pl.BlockSpec(memory_space=pltpu.VMEM)
HBM = pl.BlockSpec(memory_space=pltpu.HBM)


def call(body, outs, in_specs, scratch=(), flops=1 << 20, moved=1 << 18, place=VMEM):
    single = not isinstance(outs, (list, tuple))
    run = pl.pallas_call(
        body,
        out_shape=outs,
        in_specs=in_specs,
        out_specs=place if single else [VMEM] * len(outs),
        scratch_shapes=list(scratch),
        compiler_params=pltpu.CompilerParams(vmem_limit_bytes=16 << 20),
        cost_estimate=pl.CostEstimate(flops=flops, bytes_accessed=moved, transcendentals=0),
    )

    def bound(*args):
        return run(
            *[
                pltpu.with_memory_space_constraint(a, pltpu.HBM) if s is HBM else a
                for a, s in zip(args, in_specs)
            ]
        )

    return bound


def tables(map_ref, row, slot_ref, rank_ref, slots):
    mask = jnp.int32(0)
    for i in range(slots):
        mask = mask | (jnp.int32(1) << map_ref[row, i])
    rank = jnp.int32(0)
    for j in range(slots):
        slot_ref[rank] = jnp.int32(j)
        rank_ref[j] = rank
        rank = rank + ((mask >> j) & 1)


class Places:
    def __init__(self, levels, leaves, near_count):
        self.leaves, self.half = leaves, leaves // 2
        self.level_rows = leaves + 2 * self.half
        self.near_base = levels * self.level_rows
        self.near_count = near_count
        self.rows = -(-(self.near_base + leaves * near_count) // 8) * 8

    def piece(self, level, i):
        return level * self.level_rows + i

    def slot(self, level, k):
        return level * self.level_rows + self.leaves + k

    def slot_piece(self, level, k):
        return level * self.level_rows + self.leaves + self.half + k

    def near(self, leaf, n):
        return self.near_base + leaf * self.near_count + n


def read(table, row):
    return table[pl.ds(row, 1), :][0, 0]


def split(x):
    high = x.astype(jnp.bfloat16)
    low = (x - high.astype(jnp.float32)).astype(jnp.bfloat16)
    return jnp.concatenate([high, low], axis=0)


def times(pair, factor):
    both = jnp.dot(pair, factor, preferred_element_type=jnp.float32)
    rows = both.shape[0] // 2
    return both[:rows] + both[rows:]


def pick_lanes(blocks, high, low):
    rows = blocks[0].shape[0]
    high = jnp.broadcast_to(high, (rows, LANES))
    low = jnp.broadcast_to(low, (rows, LANES))
    out = jnp.take_along_axis(blocks[0], low, axis=1)
    for b in range(1, len(blocks)):
        out = jnp.where(high == b, jnp.take_along_axis(blocks[b], low, axis=1), out)
    return out


def column_blocks(x, leaves):
    return [x[:, b * LANES : (b + 1) * LANES].astype(jnp.float32) for b in range(leaves)]


def first_body(
    places, points, order, compress, block_map, near,
    sent, table, pts, idx, comp, maps, nears, slots, ranks, sems,
):
    leaves = idx.shape[0]
    levels = maps.shape[0]
    copies = [
        pltpu.make_async_copy(block_map, maps, sems.at[0]),
        pltpu.make_async_copy(near, nears, sems.at[1]),
        pltpu.make_async_copy(order, idx, sems.at[2]),
        pltpu.make_async_copy(points, pts, sems.at[3]),
        pltpu.make_async_copy(compress, comp, sems.at[4]),
    ]
    for copy in copies:
        copy.start()

    def put(row, value):
        table[pl.ds(row, 1), :] = jnp.full((1, LANES), value, jnp.int32)

    copies[0].wait()
    for level in range(levels):
        slot, rank = slots.at[level], ranks.at[level]
        tables(maps, level, slot, rank, leaves)
        for i in range(leaves):
            put(places.piece(level, i), rank[maps[level, i]])
        if level > 0:
            for k in range(leaves // 2):
                i = slot[k]
                put(places.slot(level, k), i)
                put(places.slot_piece(level, k), ranks[level - 1, maps[level - 1, i]])
    copies[1].wait()
    device = lax.axis_index("partner") * lax.axis_size("block") + lax.axis_index("block")
    base = device * leaves
    for leaf in range(leaves):
        for n in range(nears.shape[0]):
            put(places.near(leaf, n), nears[n, leaf] - base + REACH)
    copies[2].wait()
    copies[3].wait()
    blocks = column_blocks(pts[...], leaves)
    rows = []
    for k in range(leaves // 2):
        local = idx[pl.ds(slots[0, k], 1), :] & (leaves * LANES - 1)
        rows.append(pick_lanes(blocks, local >> 7, local & (LANES - 1)).astype(jnp.bfloat16))
    copies[4].wait()
    for k in range(leaves // 2):
        product = jnp.dot(rows[k], comp[slots[0, k]], preferred_element_type=jnp.float32)
        sent[k] = split(product)


def order_body(points, order, ordered, even, odd):
    leaves = order.shape[0]
    blocks = column_blocks(points[...], leaves)
    for leaf in range(leaves):
        local = order[pl.ds(leaf, 1), :] & (leaves * LANES - 1)
        ordered[leaf] = pick_lanes(blocks, local >> 7, local & (LANES - 1)).astype(jnp.bfloat16)
    parity = lax.axis_index("block") & 1
    head, tail = 0, leaves - REACH
    even[...] = ordered[pl.ds(jnp.where(parity == 0, tail, head), REACH)]
    odd[...] = ordered[pl.ds(jnp.where(parity == 0, head, tail), REACH)]


def prep_body(
    order, expand, mixers_in, place, joint_own, joint, mixers, sems
):
    leaves = order.shape[0]
    levels = mixers.shape[0]
    tail, rest = pl.ds(levels - 1, 1), pl.ds(0, levels - 1)
    copies = [
        pltpu.make_async_copy(mixers_in.at[part], mixers.at[part], sems.at[i])
        for i, part in enumerate((tail, rest))
    ]
    for copy in copies:
        copy.start()
    count = leaves * LANES
    target = lax.broadcasted_iota(jnp.int32, (count, LANES), 0)
    kind = lax.broadcasted_iota(jnp.int32, (8, LANES), 0)
    lane = lax.broadcasted_iota(jnp.int32, (8, LANES), 1)
    total = None
    for leaf in range(leaves):
        local = order[pl.ds(leaf, 1), :] & (count - 1)
        hit = jnp.where(target == local, 1.0, 0.0).astype(jnp.bfloat16)
        value = jnp.where(kind == 0, leaf, lane).astype(jnp.float32).astype(jnp.bfloat16)
        term = lax.dot_general(
            value, hit, (((1,), (1,)), ((), ())), preferred_element_type=jnp.float32
        )
        total = term if total is None else total + term
    place[...] = total.astype(jnp.int32)
    copies[0].wait()
    for side, out in enumerate((joint_own, joint)):
        for i in range(leaves):
            both = jnp.dot(
                mixers[mixers.shape[0] - 1, i, side], expand[i], preferred_element_type=jnp.float32
            )
            high = both.astype(jnp.bfloat16)
            out[i, :, :LANES] = high
            out[i, :, LANES:] = (both - high.astype(jnp.float32)).astype(jnp.bfloat16)
    copies[1].wait()


def top_send_body(places, table, received, factor, sent):
    for k in range(sent.shape[0]):
        i = read(table, places.slot(1, k))
        sent[k] = split(times(received[read(table, places.slot_piece(1, k))], factor[i]))


def top_own_body(places, table, received, factor, mixers, dense, own):
    for i in range(own.shape[0]):
        state = split(times(received[read(table, places.piece(0, i))], factor[i]))
        own[i] = times(state, mixers[0, i, 0])


def mix_send_body(places, level, table, received, own, mixers, sent):
    for k in range(sent.shape[0]):
        i = read(table, places.slot(level + 1, k))
        piece = received[read(table, places.slot_piece(level + 1, k))]
        sent[k] = split(own[i] + times(piece, mixers[level - 1, i, 1]))


def mix_own_body(places, level, table, received, own, mixers, own_next):
    for i in range(own.shape[0]):
        other = times(received[read(table, places.piece(level, i))], mixers[level - 1, i, 1])
        own_next[i] = times(split(own[i] + other), mixers[level, i, 0])


def times_joint(pair, joint):
    both = jnp.dot(pair, joint, preferred_element_type=jnp.float32)
    rows = both.shape[0] // 2
    return (both[:rows, :LANES] + both[rows:, :LANES]) + (both[:rows, LANES:] + both[rows:, LANES:])


def base_body(
    places, level, table, received, own, mixers, joint_own, even, ordered, odd, dense, base, windows
):
    leaves, near_count = dense.shape[0], dense.shape[1]
    parity = lax.axis_index("block") & 1
    first, last = 0, leaves + REACH
    windows[pl.ds(jnp.where(parity == 0, last, first), REACH)] = even[...]
    windows[pl.ds(jnp.where(parity == 0, first, last), REACH)] = odd[...]
    windows[pl.ds(REACH, leaves)] = ordered[...]
    for i in range(leaves):
        other = times(received[read(table, places.piece(level, i))], mixers[level - 1, i, 1])
        total = times_joint(split(own[i] + other), joint_own[i])
        source = jnp.concatenate(
            [windows[read(table, places.near(i, n))] for n in range(near_count)], axis=1
        )
        factor = dense[i].reshape(near_count * LANES, LANES)
        base[i] = total + jnp.dot(source, factor, preferred_element_type=jnp.float32)


def last_body(places, level, table, received, base, joint, place, applied, rows, sems):
    leaves = base.shape[0]
    blocks = []
    for i in range(leaves):
        piece = received[read(table, places.piece(level, i))]
        blocks.append((base[i] + times_joint(piece, joint[i])).astype(jnp.bfloat16).astype(jnp.float32))
    group = rows.shape[0] // sems.shape[0]
    copies = []
    for g in range(sems.shape[0]):
        here = slice(g * group, (g + 1) * group)
        part = [block[here] for block in blocks]
        for b in range(leaves):
            lanes = slice(b * LANES, (b + 1) * LANES)
            picked = pick_lanes(part, place[pl.ds(0, 1), lanes], place[pl.ds(1, 1), lanes])
            rows[here, lanes] = picked.astype(jnp.bfloat16)
        copies.append(pltpu.make_async_copy(rows.at[here], applied.at[here], sems.at[g]))
        copies[-1].start()
    for copy in copies:
        copy.wait()


def from_partner(x, bit):
    count = lax.axis_size("partner")
    return lax.ppermute(x, "partner", [(i, i ^ 1 << bit) for i in range(count)])


def with_neighbour(x, first):
    groups, count = lax.axis_size("partner"), lax.axis_size("block")
    to = {}
    for g in range(groups):
        for i in range(count):
            to[g * count + i] = (g ^ 1) * count + i
        for i in range(first, count - 1, 2):
            to[g * count + i], to[g * count + i + 1] = g * count + i + 1, g * count + i
    return lax.ppermute(x, ("partner", "block"), sorted(to.items()))


def on_device(
    points,
    tree_order,
    nearby_dense_blocks,
    neighbours,
    compress,
    expand,
    top_factor,
    butterfly_mixers,
    block_map,
):
    vectors, count = points.shape
    leaves, near_count = neighbours.shape
    levels = lax.axis_size("partner").bit_length() - 1
    half = leaves // 2
    places = Places(levels, leaves, near_count)
    order = tree_order.reshape(leaves, LANES)
    ints = pltpu.SMEM((levels, leaves + 1), jnp.int32)
    pair = jax.ShapeDtypeStruct((half, 2 * vectors, LANES), jnp.bfloat16)
    state = jax.ShapeDtypeStruct((leaves, vectors, LANES), jnp.float32)
    edge = jax.ShapeDtypeStruct((REACH, vectors, LANES), jnp.bfloat16)
    part = functools.partial
    assert levels > 2

    sent, table = call(
        part(first_body, places),
        [pair, jax.ShapeDtypeStruct((places.rows, LANES), jnp.int32)],
        [HBM] * 5,
        [
            pltpu.VMEM(points.shape, points.dtype),
            pltpu.VMEM(order.shape, order.dtype),
            pltpu.VMEM(compress.shape, compress.dtype),
            pltpu.SMEM(block_map.shape, block_map.dtype),
            pltpu.SMEM((near_count, leaves), neighbours.dtype),
            ints,
            ints,
            pltpu.SemaphoreType.DMA((5,)),
        ],
    )(points, order, compress, block_map, neighbours.T)
    received = from_partner(sent, levels - 1)

    ordered, even, odd = call(
        order_body,
        [jax.ShapeDtypeStruct((leaves, vectors, LANES), jnp.bfloat16), edge, edge],
        [VMEM] * 2,
        flops=1 << 24,
    )(points, order)
    even = with_neighbour(even, 0)
    odd = with_neighbour(odd, 1)

    sent = call(part(top_send_body, places), pair, [VMEM] * 3)(table, received, top_factor)
    wide = jax.ShapeDtypeStruct((leaves, LANES, 2 * LANES), jnp.bfloat16)
    place, joint_own, joint, mixers = call(
        prep_body,
        [
            jax.ShapeDtypeStruct((8, count), jnp.int32),
            wide,
            wide,
            jax.ShapeDtypeStruct(butterfly_mixers.shape, butterfly_mixers.dtype),
        ],
        [VMEM, VMEM, HBM],
        [pltpu.SemaphoreType.DMA((2,))],
        flops=1 << 24,
    )(order, expand, butterfly_mixers)
    own = call(part(top_own_body, places), state, [VMEM] * 5, flops=1 << 24)(
        table, received, top_factor, mixers, nearby_dense_blocks
    )

    for level in range(1, levels):
        received = from_partner(sent, levels - 1 - level)
        if level < levels - 1:
            sent = call(part(mix_send_body, places, level), pair, [VMEM] * 4)(
                table, received, own, mixers
            )
            if level < levels - 2:
                body, factors, scratch = mix_own_body, (mixers,), ()
            else:
                body = base_body
                factors = (mixers, joint_own, even, ordered, odd, nearby_dense_blocks)
                scratch = [pltpu.VMEM((leaves + 2 * REACH, vectors, LANES), jnp.bfloat16)]
            own = call(
                part(body, places, level),
                state,
                [VMEM] * (3 + len(factors)),
                scratch,
                flops=1 << 24,
            )(table, received, own, *factors)
    return call(
        part(last_body, places, levels - 1),
        jax.ShapeDtypeStruct(points.shape, points.dtype),
        [VMEM] * 5,
        [pltpu.VMEM(points.shape, points.dtype), pltpu.SemaphoreType.DMA((2,))],
        place=HBM,
    )(table, received, own, joint, place)


def solution(mesh):
    return jax.shard_map(
        on_device,
        mesh=mesh,
        in_specs=(
            P(None, ("partner", "block")),
            P(("partner", "block")),
            P(("partner", "block"), None, None, None),
            P(("partner", "block"), None),
            P(("partner", "block"), None, None),
            P(("partner", "block"), None, None),
            P(("partner", "block"), None, None),
            P(None, ("partner", "block"), None, None, None),
            P(),
        ),
        out_specs=P(None, ("partner", "block")),
        check_vma=False,
    )
```
